32 devices in a mesh: dp: 2 (over x), tp: 4 (over z), sp: 4 (over y, core).
Axes of the slice: x: 2, y: 2, z: 4, core: 2. Of those that a mesh axis runs over, the one named last changes fastest.
Arguments:
- hidden: bfloat16 [2048, 2048], P('dp'), parts along dimension 0
- start_pos: int32 [2], P('dp'), parts along dimension 0
- k_cache: bfloat16 [32768, 8, 128], P(('dp', 'sp'), 'tp'), parts along dimension 0
- v_cache: bfloat16 [32768, 8, 128], P(('dp', 'sp'), 'tp'), parts along dimension 0
- norm_gain: float32 [2048], replicated
- w_query: bfloat16 [2048, 2048], P(None, 'tp')
- w_key: bfloat16 [2048, 1024], P(None, 'tp')
- w_value: bfloat16 [2048, 1024], P(None, 'tp')
- q_gain: float32 [128], replicated
- k_gain: float32 [128], replicated
- w_out: bfloat16 [2048, 2048], P('tp')
Outputs:
- output 1: bfloat16 [2048, 2048], P('dp'), parts along dimension 0
- output 2: bfloat16 [32768, 8, 128], P(('dp', 'sp'), 'tp'), parts along dimension 0
- output 3: bfloat16 [32768, 8, 128], P(('dp', 'sp'), 'tp'), parts along dimension 0
There are 2 independent parts. The reference program is written for one: setup_inputs(seed, part) draws one part's arguments, and reference() takes and returns one part's arrays. A program takes and returns all parts, laid end to end along the dimension named above; an argument that names none is the same for every part.
All inputs are finite; a program needn't handle non-finite values.
Results may differ from the reference program's by a relative error of at most 0.0042618.
Values sent between devices are 32-bit elements.
A program may use at most 1 GiB of HBM per device.

```python
import math
import jax
import jax.numpy as jnp
from jax import lax

MODEL_DIM = 2048
NUM_HEADS = 16
KV_HEADS = 8
HEAD_DIM = 128
CHUNK_LEN = 1024
CACHE_LEN = 16384
START_SLACK = 2048
GROUP_SIZE = NUM_HEADS // KV_HEADS
ROPE_BASE = 1e6
NORM_EPS = 1e-6
SCORE_SPREAD = math.sqrt(max(math.log(CACHE_LEN / 16.0), 1.0))
GAIN_CENTER = math.sqrt(SCORE_SPREAD)


def setup_inputs(seed: int = 0, part: int = 0) -> dict:
    base_key = jax.random.key(seed)
    part_keys = jax.random.split(jax.random.fold_in(base_key, part), 4)
    shared_keys = jax.random.split(base_key, 7)
    q_width = NUM_HEADS * HEAD_DIM
    kv_width = KV_HEADS * HEAD_DIM
    hidden = 0.5 * jax.random.normal(part_keys[0], (CHUNK_LEN, MODEL_DIM), jnp.float32)
    lowest = CACHE_LEN - CHUNK_LEN - START_SLACK
    start_pos = jax.random.randint(part_keys[1], (1,), lowest, lowest + START_SLACK + 1, jnp.int32)
    k_cache = GAIN_CENTER * jax.random.normal(part_keys[2], (CACHE_LEN, KV_HEADS, HEAD_DIM), jnp.float32)
    v_cache = jax.random.normal(part_keys[3], (CACHE_LEN, KV_HEADS, HEAD_DIM), jnp.float32)
    norm_gain = 1.0 + 0.3 * jax.random.normal(shared_keys[0], (MODEL_DIM,), jnp.float32)
    w_query = jax.random.normal(shared_keys[1], (MODEL_DIM, q_width), jnp.float32) * MODEL_DIM ** -0.5
    w_key = jax.random.normal(shared_keys[2], (MODEL_DIM, kv_width), jnp.float32) * MODEL_DIM ** -0.5
    w_value = jax.random.normal(shared_keys[3], (MODEL_DIM, kv_width), jnp.float32) * MODEL_DIM ** -0.5
    q_gain = GAIN_CENTER * (1.0 + 0.25 * jax.random.normal(shared_keys[4], (HEAD_DIM,), jnp.float32))
    k_gain = GAIN_CENTER * (1.0 + 0.25 * jax.random.normal(shared_keys[5], (HEAD_DIM,), jnp.float32))
    w_out = jax.random.normal(shared_keys[6], (q_width, MODEL_DIM), jnp.float32) * q_width ** -0.5
    return {
        "hidden": hidden.astype(jnp.bfloat16),
        "start_pos": start_pos,
        "k_cache": k_cache.astype(jnp.bfloat16),
        "v_cache": v_cache.astype(jnp.bfloat16),
        "norm_gain": norm_gain,
        "w_query": w_query.astype(jnp.bfloat16),
        "w_key": w_key.astype(jnp.bfloat16),
        "w_value": w_value.astype(jnp.bfloat16),
        "q_gain": q_gain,
        "k_gain": k_gain,
        "w_out": w_out.astype(jnp.bfloat16),
    }


def rms_norm(values, gain):
    mean_sq = jnp.mean(values * values, axis=-1, keepdims=True)
    return values * lax.rsqrt(mean_sq + NORM_EPS) * gain


def rotary(values, positions):
    half_dim = values.shape[-1] // 2
    inv_freq = ROPE_BASE ** (-2.0 * jnp.arange(half_dim, dtype=jnp.float32) / values.shape[-1])
    angles = positions.astype(jnp.float32)[:, None] * inv_freq[None, :]
    angles = angles.reshape((positions.shape[0],) + (1,) * (values.ndim - 2) + (half_dim,))
    cosine = jnp.cos(angles)
    sine = jnp.sin(angles)
    x_first = values[..., :half_dim]
    x_second = values[..., half_dim:]
    return jnp.concatenate([x_first * cosine - x_second * sine, x_second * cosine + x_first * sine], axis=-1)


def reference(hidden, start_pos, k_cache, v_cache, norm_gain, w_query, w_key, w_value, q_gain, k_gain, w_out):
    first_pos = start_pos[0]
    positions = first_pos + jnp.arange(CHUNK_LEN, dtype=jnp.int32)
    normed = rms_norm(hidden.astype(jnp.float32), norm_gain).astype(jnp.bfloat16)
    q_proj = jnp.dot(normed, w_query, preferred_element_type=jnp.float32).reshape(CHUNK_LEN, NUM_HEADS, HEAD_DIM)
    k_proj = jnp.dot(normed, w_key, preferred_element_type=jnp.float32).reshape(CHUNK_LEN, KV_HEADS, HEAD_DIM)
    v_proj = jnp.dot(normed, w_value, preferred_element_type=jnp.float32).reshape(CHUNK_LEN, KV_HEADS, HEAD_DIM)
    q_rot = rotary(rms_norm(q_proj, q_gain), positions).astype(jnp.bfloat16)
    k_rot = rotary(rms_norm(k_proj, k_gain), positions).astype(jnp.bfloat16)
    v_new = v_proj.astype(jnp.bfloat16)
    k_full = lax.dynamic_update_slice_in_dim(k_cache, k_rot, first_pos, axis=0)
    v_full = lax.dynamic_update_slice_in_dim(v_cache, v_new, first_pos, axis=0)
    key_pos = jnp.arange(CACHE_LEN, dtype=jnp.int32)
    allowed = key_pos[None, :] <= positions[:, None]
    att_scale = HEAD_DIM ** -0.5

    def one_head(head_index):
        kv_index = head_index // GROUP_SIZE
        q_head = lax.dynamic_index_in_dim(q_rot, head_index, axis=1, keepdims=False)
        k_head = lax.dynamic_index_in_dim(k_full, kv_index, axis=1, keepdims=False)
        v_head = lax.dynamic_index_in_dim(v_full, kv_index, axis=1, keepdims=False)
        scores = jnp.dot(q_head, k_head.T, preferred_element_type=jnp.float32) * att_scale
        scores = jnp.where(allowed, scores, -jnp.inf)
        row_max = jnp.max(scores, axis=-1, keepdims=True)
        weights = jnp.exp(scores - row_max)
        numerator = jnp.dot(weights.astype(jnp.bfloat16), v_head, preferred_element_type=jnp.float32)
        denominator = jnp.sum(weights, axis=-1, keepdims=True)
        return (numerator / denominator).astype(jnp.bfloat16)

    attention = lax.map(one_head, jnp.arange(NUM_HEADS, dtype=jnp.int32))
    attention_rows = jnp.transpose(attention, (1, 0, 2)).reshape(CHUNK_LEN, NUM_HEADS * HEAD_DIM)
    head_sum = jnp.dot(attention_rows, w_out, preferred_element_type=jnp.float32)
    out = (hidden.astype(jnp.float32) + head_sum).astype(jnp.bfloat16)
    return out, k_full, v_full
```

```python
import functools

import jax
import jax.numpy as jnp
from jax import lax
from jax.experimental import pallas as pl
from jax.experimental.pallas import tpu as pltpu
from jax.sharding import PartitionSpec as P

ROPE_BASE = 1e6
NORM_EPS = 1e-6
LOG2E = 1.4426950408889634
MESH = pl.DeviceIdType.MESH
F32 = jnp.float32
BF16 = jnp.bfloat16
ROW_BLOCK = 128
STAT_ROWS = 8


def rms_norm(values, gain):
    mean_sq = jnp.mean(values * values, axis=-1, keepdims=True)
    return values * lax.rsqrt(mean_sq + NORM_EPS) * gain


def rotary(values, positions):
    half_dim = values.shape[-1] // 2
    inv_freq = ROPE_BASE ** (-2.0 * jnp.arange(half_dim, dtype=jnp.float32) / values.shape[-1])
    angles = positions.astype(jnp.float32)[:, None] * inv_freq[None, :]
    angles = angles.reshape((positions.shape[0],) + (1,) * (values.ndim - 2) + (half_dim,))
    cosine = jnp.cos(angles)
    sine = jnp.sin(angles)
    x_first = values[..., :half_dim]
    x_second = values[..., half_dim:]
    return jnp.concatenate([x_first * cosine - x_second * sine, x_second * cosine + x_first * sine], axis=-1)


def stats_tile(rows, columns):
    lane = lax.broadcasted_iota(jnp.int32, (rows, 128), 1)
    tile = jnp.zeros((rows, 128), F32)
    for k, column in enumerate(columns):
        tile = jnp.where(lane == k, column, tile)
    return tile


def stats_rows(tile):
    return jnp.transpose(tile)[:STAT_ROWS]


def stats_columns(rows8):
    return jnp.transpose(jnp.concatenate([rows8] * (128 // STAT_ROWS), axis=0))


def merge(num_a, tile_a, num_b, tile_b, scale):
    nums, columns = [], []
    for g in range(2):
        m_a, l_a = tile_a[:, 2 * g:2 * g + 1], tile_a[:, 2 * g + 1:2 * g + 2]
        m_b, l_b = tile_b[:, 2 * g:2 * g + 1], tile_b[:, 2 * g + 1:2 * g + 2]
        m = jnp.maximum(m_a, m_b)
        c_a = jnp.exp2((m_a - m) * scale)
        c_b = jnp.exp2((m_b - m) * scale)
        nums.append(num_a[:, g * 128:(g + 1) * 128] * c_a + num_b[:, g * 128:(g + 1) * 128] * c_b)
        columns += [m, l_a * c_a + l_b * c_b]
    return nums, columns


def attend_kernel(cfg, q_ref, k_ref, v_ref, bias_ref, h_ref, w_ref, out_ref, a_send, a_recv, own_num, own_st, comb_num, comb_st, y_send, y_recv,
                  y_num, y_st, o_own, o_send, o_recv, p_buf, p_recv, m_send, m_recv, f_buf, yf_recv, d1_recv, d2_recv, send_sems, recv_sems):
    nb, rb, keys, chunk_keys, chunk_len, scale, z_count = cfg
    hb = rb // 2
    dp, z, sp = lax.axis_index("dp"), lax.axis_index("tp"), lax.axis_index("sp")
    y, c = lax.div(sp, 2), lax.rem(sp, 2)
    other_y, other_c = 1 - y, 1 - c
    pair_z = z + 1 - 2 * lax.rem(z, 2)
    cross_z = z_count - 1 - z
    is_mid = jnp.logical_and(z >= 1, z <= 2)
    is_end = jnp.logical_not(is_mid)
    half_cols = w_ref.shape[1] // 2
    head_cols = w_ref.shape[0] // 2
    core_peer = (dp, z, y * 2 + other_c)
    y_peer = (dp, z, other_y * 2 + c)
    pair_peer = (dp, pair_z, sp)
    cross_peer = (dp, cross_z, sp)
    my_cols = pl.ds(pl.multiple_of(c * half_cols, half_cols), half_cols)
    peer_cols = pl.ds(pl.multiple_of(other_c * half_cols, half_cols), half_cols)

    barrier = pltpu.get_barrier_semaphore()
    for peer in (core_peer, y_peer, pair_peer):
        pl.semaphore_signal(barrier, inc=1, device_id=peer, device_id_type=MESH)

    @pl.when(is_mid)
    def _():
        pl.semaphore_signal(barrier, inc=1, device_id=cross_peer, device_id_type=MESH)
        pl.semaphore_wait(barrier, 4)

    @pl.when(is_end)
    def _():
        pl.semaphore_wait(barrier, 3)

    def copy(kind, b, src, dst, peer):
        return pltpu.make_async_remote_copy(src.at[b], dst.at[b], send_sems.at[kind, b], recv_sems.at[kind, b], device_id=peer, device_id_type=MESH)

    copy_a = lambda b: copy(0, b, a_send, a_recv, core_peer)
    copy_y = lambda b: copy(1, b, y_send, y_recv, y_peer)
    copy_o = lambda b: copy(2, b, o_send, o_recv, core_peer)
    copy_p = lambda b: copy(3, b, p_buf, p_recv, pair_peer)
    copy_m = lambda b: copy(4, b, m_send, m_recv, cross_peer)
    copy_f = lambda b: copy(5, b, f_buf, f_buf, pair_peer)
    copy_yf = lambda b: copy(6, b, f_buf, yf_recv, y_peer)
    copy_d1 = lambda b: copy(7, b, f_buf, d1_recv, core_peer)
    copy_d2 = lambda b: copy(8, b, yf_recv, d2_recv, core_peer)

    def half_rows(b, which):
        return pl.ds(pl.multiple_of(b * rb + which * hb, hb), hb)

    def attend(b, n):
        q = q_ref[n, b]
        m = l = acc = None
        row = b * rb + lax.rem(lax.broadcasted_iota(jnp.int32, (2 * rb, 1), 0), rb) + jnp.where(sp == 3, 0, keys)
        for start in range(0, keys, chunk_keys):
            s = lax.dot_general(q, k_ref[n, start:start + chunk_keys, :], (((1,), (1,)), ((), ())), preferred_element_type=F32)
            if start >= keys - chunk_len:
                column = start - (keys - chunk_len) + lax.broadcasted_iota(jnp.int32, (1, chunk_keys), 1)
                s = jnp.where(column <= row, s, -jnp.inf)
            elif start > 0:
                s = s + bias_ref[0:1, start:start + chunk_keys]
            m_new = jnp.max(s, axis=-1, keepdims=True)
            if m is not None:
                m_new = jnp.maximum(m, m_new)
            p = jnp.exp2((s - m_new) * scale)
            row_sum = jnp.sum(p, axis=-1, keepdims=True)
            pv = jnp.dot(p.astype(BF16), v_ref[n, start:start + chunk_keys, :], preferred_element_type=F32)
            if m is None:
                l, acc = row_sum, pv
            else:
                fade = jnp.exp2((m - m_new) * scale)
                l, acc = l * fade + row_sum, acc * fade + pv
            m = m_new
        tile = stats_tile(rb, [m[:rb], l[:rb], m[rb:], l[rb:]])
        return acc, tile

    def stage_attend_peer(b):
        acc, tile = attend(b, other_c)
        a_send[b, :rb, 0:128] = acc[:rb]
        a_send[b, :rb, 128:256] = acc[rb:]
        rows8 = stats_rows(tile)
        a_send[b, rb:rb + STAT_ROWS, :] = jnp.concatenate([rows8, rows8], axis=1)
        copy_a(b).start()

    def stage_attend_own(b):
        acc, tile = attend(b, c)
        own_num[:, 0:128] = acc[:rb]
        own_num[:, 128:256] = acc[rb:]
        own_st[...] = tile

    def stage_core_merge(b):
        copy_a(b).wait_recv()
        peer_tile = stats_columns(a_recv[b, rb:rb + STAT_ROWS, 0:128])
        nums, columns = merge(own_num[...], own_st[...], a_recv[b, :rb, :], peer_tile, scale)
        tile = stats_tile(rb, columns)
        comb_num[:, 0:128] = nums[0]
        comb_num[:, 128:256] = nums[1]
        comb_st[...] = tile
        mine = pl.ds(pl.multiple_of(y * hb, hb), hb)
        theirs = pl.ds(pl.multiple_of(other_y * hb, hb), hb)
        y_num[b] = comb_num[mine, :]
        y_st[b] = comb_st[mine, :]
        y_send[b, :hb, :] = comb_num[theirs, :]
        rows8 = stats_rows(tile)
        y_send[b, hb:hb + STAT_ROWS, :] = jnp.concatenate([rows8, rows8], axis=1)
        copy_y(b).start()

    def stage_y_merge(b):
        copy_y(b).wait_recv()
        comb_st[...] = stats_columns(y_recv[b, hb:hb + STAT_ROWS, 0:128])
        peer_tile = comb_st[pl.ds(pl.multiple_of(y * hb, hb), hb), :]
        nums, columns = merge(y_num[b], y_st[b], y_recv[b, :hb, :], peer_tile, scale)
        o = jnp.concatenate([nums[0] / columns[1], nums[1] / columns[3]], axis=1).astype(BF16)
        o_own[b] = o
        o_send[b] = o.astype(F32)
        copy_o(b).start()

    def stage_project(b):
        copy_o(b).wait_recv()
        w_mine = w_ref[pl.ds(pl.multiple_of(c * head_cols, head_cols), head_cols), my_cols]
        w_peer = w_ref[pl.ds(pl.multiple_of(other_c * head_cols, head_cols), head_cols), my_cols]
        part = jnp.dot(o_own[b], w_mine, preferred_element_type=F32)
        p_buf[b] = part + jnp.dot(o_recv[b].astype(BF16), w_peer, preferred_element_type=F32)

        @pl.when(is_end)
        def _():
            copy_p(b).start()

    def stage_pair_sum(b):
        copy_p(b).wait_recv()
        m_send[b] = p_buf[b] + p_recv[b]
        copy_m(b).start()

    def stage_total(b):
        copy_m(b).wait_recv()
        hidden = h_ref[half_rows(b, y), my_cols].astype(F32)
        result = (hidden + (m_send[b] + m_recv[b])).astype(BF16)
        out_ref[half_rows(b, y), my_cols] = result
        f_buf[b] = result.astype(F32)
        copy_f(b).start()
        copy_yf(b).start()
        copy_d1(b).start()

    def stage_end_total(b):
        copy_f(b).wait_recv()
        copy_yf(b).start()
        copy_d1(b).start()
        out_ref[half_rows(b, y), my_cols] = f_buf[b].astype(BF16)

    def stage_y_total(b):
        copy_yf(b).wait_recv()
        copy_d2(b).start()
        out_ref[half_rows(b, other_y), my_cols] = yf_recv[b].astype(BF16)

    def stage_store(b):
        copy_d1(b).wait_recv()
        out_ref[half_rows(b, y), peer_cols] = d1_recv[b].astype(BF16)
        copy_d2(b).wait_recv()
        out_ref[half_rows(b, other_y), peer_cols] = d2_recv[b].astype(BF16)

    def stage_sent(b):
        for sent in (copy_a, copy_y, copy_o, copy_yf, copy_d1, copy_d2):
            sent(b).wait_send()

        @pl.when(is_mid)
        def _():
            copy_m(b).wait_send()
            copy_f(b).wait_send()

        @pl.when(is_end)
        def _():
            copy_p(b).wait_send()

    def run(stage, it, lag, guard=None):
        b = it - lag
        live = jnp.logical_and(b >= 0, b < nb)
        if guard is not None:
            live = jnp.logical_and(live, guard)

        @pl.when(live)
        def _():
            stage(b)

    def body(it, carry):
        run(stage_attend_peer, it, 0)
        run(stage_store, it, 10)
        run(stage_y_total, it, 9, is_end)
        run(stage_end_total, it, 7, is_end)
        run(stage_y_total, it, 7, is_mid)
        run(stage_total, it, 5, is_mid)
        run(stage_pair_sum, it, 3, is_mid)
        run(stage_y_merge, it, 1)
        run(stage_attend_own, it, 0)
        run(stage_project, it, 1)
        run(stage_core_merge, it, 0)
        return carry

    lax.fori_loop(0, nb + 11, body, 0)
    lax.fori_loop(0, nb, lambda b, carry: (stage_sent(b), carry)[1], 0)


def attend_call(q, k_all, v_all, bias, hidden, w_out, chunk_keys, scale, z_count):
    _, nb, rows2, _ = q.shape
    rb = rows2 // 2
    hb = rb // 2
    keys = k_all.shape[1]
    chunk_len, model_dim = hidden.shape
    half_cols = model_dim // 2
    heads = w_out.shape[0] // 2
    cfg = (nb, rb, keys, chunk_keys, chunk_len, scale, z_count)
    wide = pltpu.VMEM((nb, hb, half_cols), F32)
    flops = 4 * 4 * chunk_len * keys * 128 + 2 * chunk_len * w_out.shape[0] * model_dim // 4
    return pl.pallas_call(
        functools.partial(attend_kernel, cfg),
        out_shape=jax.ShapeDtypeStruct((chunk_len, model_dim), BF16),
        in_specs=[pl.BlockSpec(memory_space=pltpu.VMEM)] * 6,
        out_specs=pl.BlockSpec(memory_space=pltpu.VMEM),
        scratch_shapes=[
            pltpu.VMEM((nb, rb + STAT_ROWS, heads), F32),
            pltpu.VMEM((nb, rb + STAT_ROWS, heads), F32),
            pltpu.VMEM((rb, heads), F32),
            pltpu.VMEM((rb, 128), F32),
            pltpu.VMEM((rb, heads), F32),
            pltpu.VMEM((rb, 128), F32),
            pltpu.VMEM((nb, hb + STAT_ROWS, heads), F32),
            pltpu.VMEM((nb, hb + STAT_ROWS, heads), F32),
            pltpu.VMEM((nb, hb, heads), F32),
            pltpu.VMEM((nb, hb, 128), F32),
            pltpu.VMEM((nb, hb, heads), BF16),
            pltpu.VMEM((nb, hb, heads), F32),
            pltpu.VMEM((nb, hb, heads), F32),
            wide, wide, wide, wide, wide, wide, wide, wide,
            pltpu.SemaphoreType.DMA((9, nb)),
            pltpu.SemaphoreType.DMA((9, nb)),
        ],
        compiler_params=pltpu.CompilerParams(collective_id=0, has_side_effects=True, vmem_limit_bytes=62 * 2**20),
        cost_estimate=pl.CostEstimate(flops=flops, bytes_accessed=16 * 2**20, transcendentals=4 * chunk_len * keys),
        name="attend",
    )(q, k_all, v_all, bias, hidden, w_out)


def solution(mesh, chunk_keys=1024):
    cache_spec = P(("dp", "sp"), "tp", None)
    in_specs = (P("dp", None), P("dp"), cache_spec, cache_spec, P(None), P(None, "tp"), P(None, "tp"), P(None, "tp"), P(None), P(None), P("tp", None))
    out_specs = (P("dp", None), cache_spec, cache_spec)

    def local_step(hidden, start_pos, k_shard, v_shard, norm_gain, w_query, w_key, w_value, q_gain, k_gain, w_out):
        chunk_len, model_dim = hidden.shape
        shard_len, kv_local, head_dim = k_shard.shape
        group_size = w_query.shape[1] // head_dim // kv_local
        first_pos = start_pos[0]
        positions = first_pos + jnp.arange(chunk_len, dtype=jnp.int32)
        normed = rms_norm(hidden.astype(jnp.float32), norm_gain).astype(jnp.bfloat16)
        q_proj = jnp.dot(normed, w_query, preferred_element_type=jnp.float32).reshape(chunk_len, kv_local, group_size, head_dim)
        k_proj = jnp.dot(normed, w_key, preferred_element_type=jnp.float32).reshape(chunk_len, kv_local, head_dim)
        v_new = jnp.dot(normed, w_value, preferred_element_type=jnp.float32).reshape(chunk_len, kv_local, head_dim).astype(jnp.bfloat16)
        q_rot = rotary(rms_norm(q_proj, q_gain), positions).astype(jnp.bfloat16)
        k_rot = rotary(rms_norm(k_proj, k_gain), positions).astype(jnp.bfloat16)
        sp = lax.axis_index("sp")
        last = sp == mesh.shape["sp"] - 1
        write_at = jnp.clip(first_pos - (mesh.shape["sp"] - 1) * shard_len, 0, shard_len - chunk_len)
        old_len = shard_len - chunk_len

        def update(shard, new_rows):
            kept = lax.dynamic_slice(shard, (write_at, 0, 0), new_rows.shape)
            updated = lax.dynamic_update_slice(shard, jnp.where(last, new_rows, kept), (write_at, 0, 0))
            seen = jnp.concatenate([shard[:old_len], jnp.where(last, new_rows, shard[old_len:])], axis=0)
            return updated, jnp.transpose(seen, (1, 0, 2))

        k_upd, k_all = update(k_shard, k_rot)
        v_upd, v_all = update(v_shard, v_new)
        key_index = jnp.arange(shard_len, dtype=jnp.int32)
        bias = jnp.where(jnp.logical_or(jnp.logical_not(last), key_index < write_at), 0.0, -jnp.inf).astype(jnp.float32)[None, :]
        n_blocks = chunk_len // ROW_BLOCK
        q_blocks = q_rot.reshape(n_blocks, ROW_BLOCK, kv_local, group_size, head_dim).transpose(2, 0, 3, 1, 4)
        q_blocks = q_blocks.reshape(kv_local, n_blocks, group_size * ROW_BLOCK, head_dim)
        out = attend_call(q_blocks, k_all, v_all, bias, hidden, w_out, chunk_keys, LOG2E * head_dim ** -0.5, mesh.shape["tp"])
        return out, k_upd, v_upd

    return jax.shard_map(local_step, mesh=mesh, in_specs=in_specs, out_specs=out_specs, check_vma=False)
```

```python
import functools

import jax
import jax.numpy as jnp
from jax import lax
from jax.experimental import pallas as pl
from jax.experimental.pallas import tpu as pltpu
from jax.sharding import PartitionSpec as P

ROPE_BASE = 1e6
NORM_EPS = 1e-6
LOG2E = 1.4426950408889634
MESH = pl.DeviceIdType.MESH
F32 = jnp.float32
BF16 = jnp.bfloat16
ROW_BLOCK = 128
STAT_ROWS = 8
SUBS = 4
LAG_Y = 6
LAG_PROJECT = 7
LAG_HOP = 3


def rotary_tables(positions, head_dim):
    half_dim = head_dim // 2
    inv_freq = ROPE_BASE ** (-2.0 * jnp.arange(half_dim, dtype=jnp.float32) / head_dim)
    lane = jnp.arange(head_dim)
    angles = positions.astype(jnp.float32)[:, None] * jnp.tile(inv_freq, 2)[None, :]
    return jnp.cos(angles), jnp.where(lane < half_dim, -1.0, 1.0)[None, :] * jnp.sin(angles)


def stats_tile(rows, columns):
    lane = lax.broadcasted_iota(jnp.int32, (rows, 128), 1)
    tile = jnp.zeros((rows, 128), F32)
    for k, column in enumerate(columns):
        tile = jnp.where(lane == k, column, tile)
    return tile


def stats_rows(tile):
    return jnp.transpose(tile)[:STAT_ROWS]


def stats_columns(rows8):
    return jnp.transpose(jnp.concatenate([rows8] * (128 // STAT_ROWS), axis=0))


def merge(num_a, tile_a, num_b, tile_b, scale):
    nums, columns = [], []
    for g in range(2):
        m_a, l_a = tile_a[:, 2 * g:2 * g + 1], tile_a[:, 2 * g + 1:2 * g + 2]
        m_b, l_b = tile_b[:, 2 * g:2 * g + 1], tile_b[:, 2 * g + 1:2 * g + 2]
        m = jnp.maximum(m_a, m_b)
        c_a = jnp.exp2((m_a - m) * scale)
        c_b = jnp.exp2((m_b - m) * scale)
        nums.append(num_a[:, g * 128:(g + 1) * 128] * c_a + num_b[:, g * 128:(g + 1) * 128] * c_b)
        columns += [m, l_a * c_a + l_b * c_b]
    return nums, columns


def attend_kernel(cfg, q_hbm, k_hbm, v_hbm, bias_ref, h_hbm, w_hbm, out_hbm, q_buf, k_buf, v_buf, h_buf, w_buf, out_buf, att_m, att_l, att_acc,
                  a_send, a_recv, own_num, own_st, comb_num, comb_st, y_send, y_recv, y_num, y_st, o_own, o_send, o_recv,
                  p_buf, p_recv, m_send, m_recv, f_buf, yf_recv, d1_recv, d2_recv, row_send, row_recv, sub_send, sub_recv, kv_sems, q_sems, h_sems, w_sem, out_sems):
    nb, rb, keys, chunk_keys, chunk_len, scale, z_count = cfg
    hb = rb // 2
    dp, z, sp = lax.axis_index("dp"), lax.axis_index("tp"), lax.axis_index("sp")
    y, c = lax.div(sp, 2), lax.rem(sp, 2)
    other_y, other_c = 1 - y, 1 - c
    pair_z = z + 1 - 2 * lax.rem(z, 2)
    cross_z = z_count - 1 - z
    is_mid = jnp.logical_and(z >= 1, z <= 2)
    is_end = jnp.logical_not(is_mid)
    half_cols = w_buf.shape[1]
    sub_cols = half_cols // SUBS
    head_cols = w_buf.shape[0] // 2
    core_peer = (dp, z, y * 2 + other_c)
    y_peer = (dp, z, other_y * 2 + c)
    pair_peer = (dp, pair_z, sp)
    cross_peer = (dp, cross_z, sp)
    my_cols = pl.ds(pl.multiple_of(c * half_cols, half_cols), half_cols)

    def kv_loads(n, half):
        span = pl.ds(half * (keys // 2), keys // 2)
        return (pltpu.make_async_copy(k_hbm.at[n, span], k_buf.at[n, span], kv_sems.at[0, n, half]),
                pltpu.make_async_copy(v_hbm.at[n, span], v_buf.at[n, span], kv_sems.at[1, n, half]))

    def q_load(n):
        return pltpu.make_async_copy(q_hbm.at[n], q_buf.at[n], q_sems.at[n])

    def half_rows(b, which):
        return pl.ds(pl.multiple_of(b * rb + which * hb, hb), hb)

    def h_load(b):
        return pltpu.make_async_copy(h_hbm.at[half_rows(b, y), my_cols], h_buf.at[b], h_sems.at[b])

    w_load = pltpu.make_async_copy(w_hbm.at[:, my_cols], w_buf, w_sem)

    for n in (other_c, c):
        q_load(n).start()
        for half in range(2):
            for load in kv_loads(n, half):
                load.start()
    w_load.start()

    @pl.when(is_mid)
    def _():
        for b in range(nb):
            h_load(b).start()

    barrier = pltpu.get_barrier_semaphore()
    for peer in (core_peer, y_peer, pair_peer):
        pl.semaphore_signal(barrier, inc=1, device_id=peer, device_id_type=MESH)

    @pl.when(is_mid)
    def _():
        pl.semaphore_signal(barrier, inc=1, device_id=cross_peer, device_id_type=MESH)
        pl.semaphore_wait(barrier, 4)

    @pl.when(is_end)
    def _():
        pl.semaphore_wait(barrier, 3)

    def row_copy(kind, b, src, dst, peer):
        return pltpu.make_async_remote_copy(src.at[b], dst.at[b], row_send.at[kind, b], row_recv.at[kind, b], device_id=peer, device_id_type=MESH)

    def sub_copy(kind, b, j, src, dst, peer):
        return pltpu.make_async_remote_copy(src.at[b, j], dst.at[b, j], sub_send.at[kind, b, j], sub_recv.at[kind, b, j], device_id=peer, device_id_type=MESH)

    copy_a = lambda b: row_copy(0, b, a_send, a_recv, core_peer)
    copy_y = lambda b: row_copy(1, b, y_send, y_recv, y_peer)
    copy_o = lambda b: row_copy(2, b, o_send, o_recv, core_peer)
    copy_p = lambda b, j: sub_copy(0, b, j, p_buf, p_recv, pair_peer)
    copy_m = lambda b, j: sub_copy(1, b, j, m_send, m_recv, cross_peer)
    copy_f = lambda b, j: sub_copy(2, b, j, f_buf, f_buf, pair_peer)
    copy_yf = lambda b, j: sub_copy(3, b, j, f_buf, yf_recv, y_peer)
    copy_d1 = lambda b, j: sub_copy(4, b, j, f_buf, d1_recv, core_peer)
    copy_d2 = lambda b, j: sub_copy(5, b, j, yf_recv, d2_recv, core_peer)

    def out_store(b):
        rows = pl.ds(pl.multiple_of(b * rb, rb), rb)
        return pltpu.make_async_copy(out_buf.at[rows], out_hbm.at[rows], out_sems.at[b])

    def columns_of(core, j):
        return pl.ds(pl.multiple_of(core * half_cols + j * sub_cols, sub_cols), sub_cols)

    def attend(b, n, half):
        q = q_buf[n, b]
        if half:
            m, l, acc = att_m[...], att_l[...], att_acc[...]
        else:
            m = l = acc = None
        row = b * rb + lax.rem(lax.broadcasted_iota(jnp.int32, (2 * rb, 1), 0), rb) + jnp.where(sp == 3, 0, keys)
        for start in range(half * (keys // 2), (half + 1) * (keys // 2), chunk_keys):
            s = lax.dot_general(q, k_buf[n, start:start + chunk_keys, :], (((1,), (1,)), ((), ())), preferred_element_type=F32)
            if start >= keys - chunk_len:
                column = start - (keys - chunk_len) + lax.broadcasted_iota(jnp.int32, (1, chunk_keys), 1)
                s = jnp.where(column <= row, s, -jnp.inf)
            elif start > 0:
                s = s + bias_ref[0:1, start:start + chunk_keys]
            m_new = jnp.max(s, axis=-1, keepdims=True)
            if m is not None:
                m_new = jnp.maximum(m, m_new)
            p = jnp.exp2((s - m_new) * scale)
            row_sum = jnp.sum(p, axis=-1, keepdims=True)
            pv = jnp.dot(p.astype(BF16), v_buf[n, start:start + chunk_keys, :], preferred_element_type=F32)
            if m is None:
                l, acc = row_sum, pv
            else:
                fade = jnp.exp2((m - m_new) * scale)
                l, acc = l * fade + row_sum, acc * fade + pv
            m = m_new
        if not half:
            att_m[...], att_l[...], att_acc[...] = m, l, acc
        return acc, m, l

    def stage_attend(b, piece):
        head, half = piece // 2, piece % 2
        n = c if head else other_c

        @pl.when(b == 0)
        def _():
            if half == 0:
                q_load(n).wait()
            for load in kv_loads(n, half):
                load.wait()

        acc, m, l = attend(b, n, half)
        if not half:
            return
        tile = stats_tile(rb, [m[:rb], l[:rb], m[rb:], l[rb:]])
        if head:
            own_num[:, 0:128] = acc[:rb]
            own_num[:, 128:256] = acc[rb:]
            own_st[...] = tile
        else:
            a_send[b, :rb, 0:128] = acc[:rb]
            a_send[b, :rb, 128:256] = acc[rb:]
            rows8 = stats_rows(tile)
            a_send[b, rb:rb + STAT_ROWS, :] = jnp.concatenate([rows8, rows8], axis=1)
            copy_a(b).start()

    def stage_core_merge(b):
        copy_a(b).wait_recv()
        peer_tile = stats_columns(a_recv[b, rb:rb + STAT_ROWS, 0:128])
        nums, columns = merge(own_num[...], own_st[...], a_recv[b, :rb, :], peer_tile, scale)
        tile = stats_tile(rb, columns)
        comb_num[:, 0:128] = nums[0]
        comb_num[:, 128:256] = nums[1]
        comb_st[...] = tile
        mine = pl.ds(pl.multiple_of(y * hb, hb), hb)
        theirs = pl.ds(pl.multiple_of(other_y * hb, hb), hb)
        y_send[b, :hb, :] = comb_num[theirs, :]
        rows8 = stats_rows(tile)
        y_send[b, hb:hb + STAT_ROWS, :] = jnp.concatenate([rows8, rows8], axis=1)
        copy_y(b).start()
        y_num[b] = comb_num[mine, :]
        y_st[b] = comb_st[mine, :]

    def stage_y_merge(b):
        copy_y(b).wait_recv()
        comb_st[...] = stats_columns(y_recv[b, hb:hb + STAT_ROWS, 0:128])
        peer_tile = comb_st[pl.ds(pl.multiple_of(y * hb, hb), hb), :]
        nums, columns = merge(y_num[b], y_st[b], y_recv[b, :hb, :], peer_tile, scale)
        o = jnp.concatenate([nums[0] / columns[1], nums[1] / columns[3]], axis=1).astype(BF16)
        o_send[b] = o.astype(F32)
        copy_o(b).start()
        o_own[b] = o

    def stage_project(b):
        @pl.when(b == 0)
        def _():
            w_load.wait()

        copy_o(b).wait_recv()
        w_mine = w_buf[pl.ds(pl.multiple_of(c * head_cols, head_cols), head_cols), :]
        w_peer = w_buf[pl.ds(pl.multiple_of(other_c * head_cols, head_cols), head_cols), :]
        part = jnp.dot(o_own[b], w_mine, preferred_element_type=F32)
        part = part + jnp.dot(o_recv[b].astype(BF16), w_peer, preferred_element_type=F32)
        for j in range(SUBS):
            p_buf[b, j] = part[:, j * sub_cols:(j + 1) * sub_cols]

        @pl.when(is_end)
        def _():
            for j in range(SUBS):
                copy_p(b, j).start()

    def stage_pair_sum(b, j):
        copy_p(b, j).wait_recv()
        m_send[b, j] = p_buf[b, j] + p_recv[b, j]
        copy_m(b, j).start()

    def stage_total(b, j):
        if j == 0:
            h_load(b).wait()
        copy_m(b, j).wait_recv()
        hidden = h_buf[b, :, j * sub_cols:(j + 1) * sub_cols].astype(F32)
        result = (hidden + (m_send[b, j] + m_recv[b, j])).astype(BF16)
        f_buf[b, j] = result.astype(F32)
        copy_f(b, j).start()
        copy_yf(b, j).start()
        copy_d1(b, j).start()
        out_buf[half_rows(b, y), columns_of(c, j)] = result

    def stage_end_total(b, j):
        copy_f(b, j).wait_recv()
        copy_yf(b, j).start()
        copy_d1(b, j).start()
        out_buf[half_rows(b, y), columns_of(c, j)] = f_buf[b, j].astype(BF16)

    def stage_y_total(b, j):
        copy_yf(b, j).wait_recv()
        copy_d2(b, j).start()
        out_buf[half_rows(b, other_y), columns_of(c, j)] = yf_recv[b, j].astype(BF16)

    def stage_store(b, j):
        copy_d1(b, j).wait_recv()
        out_buf[half_rows(b, y), columns_of(other_c, j)] = d1_recv[b, j].astype(BF16)
        copy_d2(b, j).wait_recv()
        out_buf[half_rows(b, other_y), columns_of(other_c, j)] = d2_recv[b, j].astype(BF16)
        if j == SUBS - 1:
            out_store(b).start()

    def stage_sent(b):
        for sent in (copy_a, copy_y, copy_o):
            sent(b).wait_send()
        out_store(b).wait()
        for j in range(SUBS):
            for sent in (copy_yf, copy_d1, copy_d2):
                sent(b, j).wait_send()

        @pl.when(is_mid)
        def _():
            for j in range(SUBS):
                copy_m(b, j).wait_send()
                copy_f(b, j).wait_send()

        @pl.when(is_end)
        def _():
            for j in range(SUBS):
                copy_p(b, j).wait_send()

    def run(stage, it, step, lag, guard=None, sub=True):
        j = (step - lag) % SUBS
        if not sub and j:
            return
        b = it + (step - lag - j) // SUBS
        live = jnp.logical_and(b >= 0, b < nb)
        if guard is not None:
            live = jnp.logical_and(live, guard)

        @pl.when(live)
        def _():
            if sub:
                stage(b, j)
            else:
                stage(b)

    lag_p, hop = LAG_PROJECT + LAG_HOP, LAG_HOP
    lag_store = lag_p + 3 * hop + 2

    def body(it, carry):
        for step in range(SUBS):
            run(stage_store, it, step, lag_store)
            run(stage_y_total, it, step, lag_p + 3 * hop, is_end)
            run(stage_end_total, it, step, lag_p + 2 * hop, is_end)
            run(stage_y_total, it, step, lag_p + 2 * hop, is_mid)
            run(stage_total, it, step, lag_p + hop, is_mid)
            run(stage_pair_sum, it, step, lag_p, is_mid)
            run(stage_attend, it, step, 0)
            run(stage_core_merge, it, step, SUBS - 1, sub=False)
            run(stage_y_merge, it, step, LAG_Y, sub=False)
            run(stage_project, it, step, LAG_PROJECT, sub=False)
        return carry

    lax.fori_loop(0, nb + (lag_store + SUBS - 1) // SUBS, body, 0)
    lax.fori_loop(0, nb, lambda b, carry: (stage_sent(b), carry)[1], 0)


def prep_kernel(cfg, pos_ref, h_hbm, gain_ref, wq_hbm, wk_hbm, wv_hbm, qg_ref, kg_ref, cos_ref, sin_ref, kc_hbm, vc_hbm,
                q_out, k_out, v_out, kc_out, vc_out, h_buf, normed, wq_buf, wkv_buf, kc_buf, vc_buf, new_buf, in_sems, cache_sems, out_sems):
    nb, rb, last_index, old_len = cfg
    chunk_len, _ = h_buf.shape
    shard_len = kc_buf.shape[0]
    kv_cols = wk_hbm.shape[1]
    is_last = lax.axis_index("sp") == last_index
    write_at = jnp.clip(pos_ref[0] - last_index * shard_len, 0, shard_len - chunk_len)
    parts = 4
    rows = chunk_len // parts

    def load(k, src, dst):
        return pltpu.make_async_copy(src, dst, in_sems.at[k])

    h_loads = [load(k, h_hbm.at[pl.ds(k * rows, rows)], h_buf.at[pl.ds(k * rows, rows)]) for k in range(parts)]
    wq_load = load(parts, wq_hbm, wq_buf)
    wk_load = load(parts + 1, wk_hbm, wkv_buf.at[:, pl.ds(0, kv_cols)])
    wv_load = load(parts + 2, wv_hbm, wkv_buf.at[:, pl.ds(kv_cols, kv_cols)])
    kc_load = pltpu.make_async_copy(kc_hbm, kc_buf, cache_sems.at[0])
    vc_load = pltpu.make_async_copy(vc_hbm, vc_buf, cache_sems.at[1])
    kc_store = pltpu.make_async_copy(kc_buf, kc_out, out_sems.at[0])
    vc_store = pltpu.make_async_copy(vc_buf, vc_out, out_sems.at[1])
    h_loads[0].start()
    kc_load.start()
    wq_load.start()
    for k in range(1, parts):
        h_loads[k].start()
    vc_load.start()

    @pl.when(is_last)
    def _():
        wk_load.start()
        wv_load.start()

    def normalize(x, gain):
        return x * lax.rsqrt(jnp.mean(x * x, axis=-1, keepdims=True) + NORM_EPS) * gain

    def rotate(x, part):
        return x * cos_ref[part * rows:(part + 1) * rows, :] + pltpu.roll(x, 64, 1) * sin_ref[part * rows:(part + 1) * rows, :]

    def split_heads(buf, out, start, stop):
        for row in range(start, stop, 256):
            x = buf[row:row + 256].reshape(256, kv_cols)
            for n in range(2):
                out[n, row:row + 256, :] = x[:, n * 128:(n + 1) * 128]

    def project_q(part):
        x = h_buf[part * rows:(part + 1) * rows, :].astype(F32)
        norm = normalize(x, gain_ref[...]).astype(BF16)
        normed[part * rows:(part + 1) * rows, :] = norm
        proj = jnp.dot(norm, wq_buf[...], preferred_element_type=F32)
        for head in range(4):
            n, g = head // 2, head % 2
            rot = rotate(normalize(proj[:, head * 128:(head + 1) * 128], qg_ref[...]), part).astype(BF16)
            for sub in range(rows // rb):
                q_out[n, part * (rows // rb) + sub, g * rb:(g + 1) * rb, :] = rot[sub * rb:(sub + 1) * rb]

    h_loads[0].wait()
    wq_load.wait()
    project_q(0)
    kc_load.wait()
    kc_store.start()
    split_heads(kc_buf, k_out, 0, old_len)
    for part in range(1, parts):
        h_loads[part].wait()
        project_q(part)
    vc_load.wait()
    vc_store.start()
    split_heads(vc_buf, v_out, 0, old_len)

    @pl.when(jnp.logical_not(is_last))
    def _():
        split_heads(kc_buf, k_out, old_len, shard_len)
        split_heads(vc_buf, v_out, old_len, shard_len)
        kc_store.wait()
        vc_store.wait()

    @pl.when(is_last)
    def _():
        wk_load.wait()
        wv_load.wait()
        for part in range(parts):
            span = slice(part * rows, (part + 1) * rows)
            proj = jnp.dot(normed[span, :], wkv_buf[...], preferred_element_type=F32)
            heads = []
            for n in range(2):
                heads.append(rotate(normalize(proj[:, n * 128:(n + 1) * 128], kg_ref[...]), part).astype(BF16))
                k_out[n, old_len + part * rows:old_len + (part + 1) * rows, :] = heads[n]
                v_out[n, old_len + part * rows:old_len + (part + 1) * rows, :] = proj[:, kv_cols + n * 128:kv_cols + (n + 1) * 128].astype(BF16)
            new_buf[0, span] = jnp.concatenate(heads, axis=1).reshape(rows, 2, 128)
            new_buf[1, span] = proj[:, kv_cols:].astype(BF16).reshape(rows, 2, 128)
        kc_store.wait()
        vc_store.wait()
        k_store = pltpu.make_async_copy(new_buf.at[0], kc_out.at[pl.ds(write_at, chunk_len)], out_sems.at[0])
        v_store = pltpu.make_async_copy(new_buf.at[1], vc_out.at[pl.ds(write_at, chunk_len)], out_sems.at[1])
        k_store.start()
        v_store.start()
        k_store.wait()
        v_store.wait()


def prep_call(start_pos, hidden, norm_gain, w_query, w_key, w_value, q_gain, k_gain, cosine, sine, k_shard, v_shard, last_index):
    chunk_len, model_dim = hidden.shape
    shard_len, kv_local, head_dim = k_shard.shape
    nb = chunk_len // ROW_BLOCK
    vmem = pl.BlockSpec(memory_space=pltpu.VMEM)
    hbm = pl.BlockSpec(memory_space=pl.ANY)
    cfg = (nb, ROW_BLOCK, last_index, shard_len - chunk_len)
    kv_shape = jax.ShapeDtypeStruct((kv_local, shard_len, head_dim), BF16)
    cache_shape = jax.ShapeDtypeStruct(k_shard.shape, BF16)
    return pl.pallas_call(
        functools.partial(prep_kernel, cfg),
        out_shape=(jax.ShapeDtypeStruct((kv_local, nb, 2 * ROW_BLOCK, head_dim), BF16), kv_shape, kv_shape, cache_shape, cache_shape),
        in_specs=[pl.BlockSpec(memory_space=pltpu.SMEM), hbm, vmem, hbm, hbm, hbm, vmem, vmem, vmem, vmem, hbm, hbm],
        out_specs=(vmem, vmem, vmem, hbm, hbm),
        scratch_shapes=[
            pltpu.VMEM((chunk_len, model_dim), BF16),
            pltpu.VMEM((chunk_len, model_dim), BF16),
            pltpu.VMEM(w_query.shape, BF16),
            pltpu.VMEM((model_dim, 2 * w_key.shape[1]), BF16),
            pltpu.VMEM(k_shard.shape, BF16),
            pltpu.VMEM(k_shard.shape, BF16),
            pltpu.VMEM((2, chunk_len, kv_local, head_dim), BF16),
            pltpu.SemaphoreType.DMA((7,)),
            pltpu.SemaphoreType.DMA((2,)),
            pltpu.SemaphoreType.DMA((2,)),
        ],
        compiler_params=pltpu.CompilerParams(vmem_limit_bytes=48 * 2**20),
        cost_estimate=pl.CostEstimate(flops=2 * chunk_len * model_dim * 1024, bytes_accessed=24 * 2**20, transcendentals=0),
        name="prep",
    )(start_pos, hidden, norm_gain[None, :], w_query, w_key, w_value, q_gain[None, :], k_gain[None, :], cosine, sine, k_shard, v_shard)


def attend_call(q, k_all, v_all, bias, hidden, w_out, chunk_keys, scale, z_count):
    _, nb, rows2, _ = q.shape
    rb = rows2 // 2
    hb = rb // 2
    keys = k_all.shape[1]
    chunk_len, model_dim = hidden.shape
    half_cols = model_dim // 2
    heads = w_out.shape[0] // 2
    cfg = (nb, rb, keys, chunk_keys, chunk_len, scale, z_count)
    sub = pltpu.VMEM((nb, SUBS, hb, half_cols // SUBS), F32)
    flops = 4 * 4 * chunk_len * keys * 128 + 2 * chunk_len * w_out.shape[0] * model_dim // 4
    vmem = pl.BlockSpec(memory_space=pltpu.VMEM)
    hbm = pl.BlockSpec(memory_space=pl.ANY)
    return pl.pallas_call(
        functools.partial(attend_kernel, cfg),
        out_shape=jax.ShapeDtypeStruct((chunk_len, model_dim), BF16),
        in_specs=[hbm, hbm, hbm, vmem, hbm, hbm],
        out_specs=hbm,
        scratch_shapes=[
            pltpu.VMEM(q.shape, BF16),
            pltpu.VMEM(k_all.shape, BF16),
            pltpu.VMEM(v_all.shape, BF16),
            pltpu.VMEM((nb, hb, half_cols), BF16),
            pltpu.VMEM((w_out.shape[0], half_cols), BF16),
            pltpu.VMEM((chunk_len, model_dim), BF16),
            pltpu.VMEM((2 * rb, 1), F32),
            pltpu.VMEM((2 * rb, 1), F32),
            pltpu.VMEM((2 * rb, 128), F32),
            pltpu.VMEM((nb, rb + STAT_ROWS, heads), F32),
            pltpu.VMEM((nb, rb + STAT_ROWS, heads), F32),
            pltpu.VMEM((rb, heads), F32),
            pltpu.VMEM((rb, 128), F32),
            pltpu.VMEM((rb, heads), F32),
            pltpu.VMEM((rb, 128), F32),
            pltpu.VMEM((nb, hb + STAT_ROWS, heads), F32),
            pltpu.VMEM((nb, hb + STAT_ROWS, heads), F32),
            pltpu.VMEM((nb, hb, heads), F32),
            pltpu.VMEM((nb, hb, 128), F32),
            pltpu.VMEM((nb, hb, heads), BF16),
            pltpu.VMEM((nb, hb, heads), F32),
            pltpu.VMEM((nb, hb, heads), F32),
            sub, sub, sub, sub, sub, sub, sub, sub,
            pltpu.SemaphoreType.DMA((3, nb)),
            pltpu.SemaphoreType.DMA((3, nb)),
            pltpu.SemaphoreType.DMA((6, nb, SUBS)),
            pltpu.SemaphoreType.DMA((6, nb, SUBS)),
            pltpu.SemaphoreType.DMA((2, 2, 2)),
            pltpu.SemaphoreType.DMA((2,)),
            pltpu.SemaphoreType.DMA((nb,)),
            pltpu.SemaphoreType.DMA,
            pltpu.SemaphoreType.DMA((nb,)),
        ],
        compiler_params=pltpu.CompilerParams(collective_id=0, has_side_effects=True, vmem_limit_bytes=56 * 2**20),
        cost_estimate=pl.CostEstimate(flops=flops, bytes_accessed=16 * 2**20, transcendentals=4 * chunk_len * keys),
        name="attend",
    )(q, k_all, v_all, bias, hidden, w_out)


def solution(mesh, chunk_keys=1024):
    cache_spec = P(("dp", "sp"), "tp", None)
    in_specs = (P("dp", None), P("dp"), cache_spec, cache_spec, P(None), P(None, "tp"), P(None, "tp"), P(None, "tp"), P(None), P(None), P("tp", None))
    out_specs = (P("dp", None), cache_spec, cache_spec)

    def local_step(hidden, start_pos, k_shard, v_shard, norm_gain, w_query, w_key, w_value, q_gain, k_gain, w_out):
        chunk_len, model_dim = hidden.shape
        shard_len, kv_local, head_dim = k_shard.shape
        last_index = mesh.shape["sp"] - 1
        positions = start_pos[0] + jnp.arange(chunk_len, dtype=jnp.int32)
        cosine, sine = rotary_tables(positions, head_dim)
        q_blocks, k_all, v_all, k_upd, v_upd = prep_call(start_pos, hidden, norm_gain, w_query, w_key, w_value, q_gain, k_gain, cosine, sine, k_shard, v_shard, last_index)
        key_index = jnp.arange(shard_len, dtype=jnp.int32)
        seen = jnp.logical_or(lax.axis_index("sp") != last_index, key_index < start_pos[0] - last_index * shard_len)
        bias = jnp.where(seen, 0.0, -jnp.inf).astype(jnp.float32)[None, :]
        out = attend_call(q_blocks, k_all, v_all, bias, hidden, w_out, chunk_keys, LOG2E * head_dim ** -0.5, mesh.shape["tp"])
        return out, k_upd, v_upd

    return jax.shard_map(local_step, mesh=mesh, in_specs=in_specs, out_specs=out_specs, check_vma=False)
```

```python
import functools

import jax
import jax.numpy as jnp
from jax import lax
from jax.experimental import pallas as pl
from jax.experimental.pallas import tpu as pltpu
from jax.sharding import PartitionSpec as P

ROPE_BASE = 1e6
NORM_EPS = 1e-6
LOG2E = 1.4426950408889634
MESH = pl.DeviceIdType.MESH
F32 = jnp.float32
BF16 = jnp.bfloat16
ROW_BLOCK = 128
STAT_ROWS = 8
SUBS = 4
LAG_Y = 6
LAG_PROJECT = 7
LAG_HOP = 3
LAST_SHARD = 3


def rotary_tables(positions, head_dim):
    half_dim = head_dim // 2
    inv_freq = ROPE_BASE ** (-2.0 * jnp.arange(half_dim, dtype=jnp.float32) / head_dim)
    lane = jnp.arange(head_dim)
    angles = positions.astype(jnp.float32)[:, None] * jnp.tile(inv_freq, 2)[None, :]
    return jnp.cos(angles), jnp.where(lane < half_dim, -1.0, 1.0)[None, :] * jnp.sin(angles)


def stats_tile(rows, columns):
    lane = lax.broadcasted_iota(jnp.int32, (rows, 128), 1)
    tile = jnp.zeros((rows, 128), F32)
    for k, column in enumerate(columns):
        tile = jnp.where(lane == k, column, tile)
    return tile


def stats_rows(tile):
    return jnp.transpose(tile)[:STAT_ROWS]


def stats_columns(rows8):
    return jnp.transpose(jnp.concatenate([rows8] * (128 // STAT_ROWS), axis=0))


def merge(num_a, tile_a, num_b, tile_b, scale):
    nums, columns = [], []
    for g in range(2):
        m_a, l_a = tile_a[:, 2 * g:2 * g + 1], tile_a[:, 2 * g + 1:2 * g + 2]
        m_b, l_b = tile_b[:, 2 * g:2 * g + 1], tile_b[:, 2 * g + 1:2 * g + 2]
        m = jnp.maximum(m_a, m_b)
        c_a = jnp.exp2((m_a - m) * scale)
        c_b = jnp.exp2((m_b - m) * scale)
        nums.append(num_a[:, g * 128:(g + 1) * 128] * c_a + num_b[:, g * 128:(g + 1) * 128] * c_b)
        columns += [m, l_a * c_a + l_b * c_b]
    return nums, columns


def attend_kernel(cfg, pos_ref, h_hbm, gain_ref, wq_hbm, wk_hbm, wv_hbm, qg_ref, kg_ref, cos_ref, sin_ref, kc_hbm, vc_hbm, w_hbm, out_hbm, kn_hbm, vn_hbm,
                  h_buf, wq_buf, wkv_buf, kc_buf, vc_buf, k_buf, v_buf, new_buf, q_buf, bias_ref, w_buf, out_buf, att_m, att_l, att_acc,
                  a_send, a_recv, own_num, own_st, comb_num, comb_st, y_send, y_recv, y_num, y_st, o_own, o_send, o_recv,
                  p_buf, p_recv, m_send, m_recv, f_buf, yf_recv, d1_recv, d2_recv, row_send, row_recv, sub_send, sub_recv,
                  kv_sems, w_sems, h_sems, new_sems, out_sems):
    nb, rb, keys, chunk_keys, chunk_len, scale, z_count = cfg
    hb = rb // 2
    dp, z, sp = lax.axis_index("dp"), lax.axis_index("tp"), lax.axis_index("sp")
    y, c = lax.div(sp, 2), lax.rem(sp, 2)
    other_y, other_c = 1 - y, 1 - c
    pair_z = z + 1 - 2 * lax.rem(z, 2)
    cross_z = z_count - 1 - z
    is_mid = jnp.logical_and(z >= 1, z <= 2)
    is_end = jnp.logical_not(is_mid)
    half_cols = w_buf.shape[1]
    sub_cols = half_cols // SUBS
    head_cols = w_buf.shape[0] // 2
    core_peer = (dp, z, y * 2 + other_c)
    y_peer = (dp, z, other_y * 2 + c)
    pair_peer = (dp, pair_z, sp)
    cross_peer = (dp, cross_z, sp)
    my_cols = pl.ds(pl.multiple_of(c * half_cols, half_cols), half_cols)

    last = sp == LAST_SHARD
    old_len = keys - chunk_len
    kv_cols = wk_hbm.shape[1]
    limit = jnp.where(last, pos_ref[0] - LAST_SHARD * keys, keys)

    def half_rows(b, which):
        return pl.ds(pl.multiple_of(b * rb + which * hb, hb), hb)

    def block_rows(b, rows):
        return pl.ds(pl.multiple_of(b * rows, rows), rows)

    def cache_loads(half):
        span = pl.ds(half * (keys // 2), keys // 2)
        return (pltpu.make_async_copy(kc_hbm.at[span], kc_buf.at[span], kv_sems.at[0, half]),
                pltpu.make_async_copy(vc_hbm.at[span], vc_buf.at[span], kv_sems.at[1, half]))

    def h_load(b):
        return pltpu.make_async_copy(h_hbm.at[block_rows(b, rb)], h_buf.at[block_rows(b, rb)], h_sems.at[b])

    wq_load = pltpu.make_async_copy(wq_hbm, wq_buf, w_sems.at[0])
    wk_load = pltpu.make_async_copy(wk_hbm, wkv_buf.at[:, pl.ds(0, kv_cols)], w_sems.at[1])
    wv_load = pltpu.make_async_copy(wv_hbm, wkv_buf.at[:, pl.ds(kv_cols, kv_cols)], w_sems.at[2])
    w_load = pltpu.make_async_copy(w_hbm.at[:, my_cols], w_buf, w_sems.at[3])
    kn_store = pltpu.make_async_copy(new_buf.at[0], kn_hbm, new_sems.at[0])
    vn_store = pltpu.make_async_copy(new_buf.at[1], vn_hbm, new_sems.at[1])

    @pl.when(last)
    def _():
        wk_load.start()
        wv_load.start()

    h_load(0).start()
    h_load(1).start()
    wq_load.start()
    for half in range(2):
        for load in cache_loads(half):
            load.start()
    for b in range(2, nb):
        h_load(b).start()
    w_load.start()

    barrier = pltpu.get_barrier_semaphore()
    for peer in (core_peer, y_peer, pair_peer):
        pl.semaphore_signal(barrier, inc=1, device_id=peer, device_id_type=MESH)

    @pl.when(is_mid)
    def _():
        pl.semaphore_signal(barrier, inc=1, device_id=cross_peer, device_id_type=MESH)
        pl.semaphore_wait(barrier, 4)

    @pl.when(is_end)
    def _():
        pl.semaphore_wait(barrier, 3)

    key_index = lax.broadcasted_iota(jnp.int32, (1, keys), 1)
    bias_ref[...] = jnp.where(key_index < limit, 0.0, -jnp.inf).astype(F32)

    def normalize(x, gain):
        return x * lax.rsqrt(jnp.mean(x * x, axis=-1, keepdims=True) + NORM_EPS) * gain

    def rotate(x, span):
        return (x * cos_ref[span, :] + pltpu.roll(x, 64, 1) * sin_ref[span, :]).astype(BF16)

    def project_q(b):
        @pl.when(jnp.logical_not(last))
        def _():
            h_load(b).wait()

        @pl.when(b == 0)
        def _():
            wq_load.wait()

        span = block_rows(b, rb)
        normed = normalize(h_buf[span, :].astype(F32), gain_ref[...]).astype(BF16)
        proj = jnp.dot(normed, wq_buf[...], preferred_element_type=F32)
        for head in range(4):
            q_buf[head // 2, (head % 2) * rb:(head % 2 + 1) * rb, :] = rotate(normalize(proj[:, head * 128:(head + 1) * 128], qg_ref[...]), span)

    def project_new(part, carry):
        rows = 2 * rb
        for b in range(2):
            h_load(2 * part + b).wait()
        span = block_rows(part, rows)
        normed = normalize(h_buf[span, :].astype(F32), gain_ref[...]).astype(BF16)
        proj = jnp.dot(normed, wkv_buf[...], preferred_element_type=F32)
        place = pl.ds(pl.multiple_of(old_len + part * rows, rows), rows)
        heads = []
        for n in range(2):
            heads.append(rotate(normalize(proj[:, n * 128:(n + 1) * 128], kg_ref[...]), span))
            k_buf[n, place, :] = heads[n]
            v_buf[n, place, :] = proj[:, kv_cols + n * 128:kv_cols + (n + 1) * 128].astype(BF16)
        new_buf[0, span] = jnp.concatenate(heads, axis=1).reshape(rows, 2, 128)
        new_buf[1, span] = proj[:, kv_cols:].astype(BF16).reshape(rows, 2, 128)
        return carry

    def split_heads(start, stop):
        for src, dst in ((kc_buf, k_buf), (vc_buf, v_buf)):
            for row in range(start, stop, 256):
                x = src[row:row + 256].reshape(256, kv_cols)
                for n in range(2):
                    dst[n, row:row + 256, :] = x[:, n * 128:(n + 1) * 128]

    def prepare_keys(half):
        for load in cache_loads(half):
            load.wait()
        if half == 0:
            split_heads(0, keys // 2)
        else:
            split_heads(keys // 2, old_len)

            @pl.when(jnp.logical_not(last))
            def _():
                split_heads(old_len, keys)

    @pl.when(last)
    def _():
        wk_load.wait()
        wv_load.wait()
        lax.fori_loop(0, chunk_len // (2 * rb), project_new, 0)
        kn_store.start()
        vn_store.start()

    def row_copy(kind, b, src, dst, peer):
        return pltpu.make_async_remote_copy(src.at[b], dst.at[b], row_send.at[kind, b], row_recv.at[kind, b], device_id=peer, device_id_type=MESH)

    def sub_copy(kind, b, j, src, dst, peer):
        return pltpu.make_async_remote_copy(src.at[b, j], dst.at[b, j], sub_send.at[kind, b, j], sub_recv.at[kind, b, j], device_id=peer, device_id_type=MESH)

    copy_a = lambda b: row_copy(0, b, a_send, a_recv, core_peer)
    copy_y = lambda b: row_copy(1, b, y_send, y_recv, y_peer)
    copy_o = lambda b: row_copy(2, b, o_send, o_recv, core_peer)
    copy_p = lambda b, j: sub_copy(0, b, j, p_buf, p_recv, pair_peer)
    copy_m = lambda b, j: sub_copy(1, b, j, m_send, m_recv, cross_peer)
    copy_f = lambda b, j: sub_copy(2, b, j, f_buf, f_buf, pair_peer)
    copy_yf = lambda b, j: sub_copy(3, b, j, f_buf, yf_recv, y_peer)
    copy_d1 = lambda b, j: sub_copy(4, b, j, f_buf, d1_recv, core_peer)
    copy_d2 = lambda b, j: sub_copy(5, b, j, yf_recv, d2_recv, core_peer)

    def out_store(b):
        rows = pl.ds(pl.multiple_of(b * rb, rb), rb)
        return pltpu.make_async_copy(out_buf.at[rows], out_hbm.at[rows], out_sems.at[b])

    def columns_of(core, j):
        return pl.ds(pl.multiple_of(core * half_cols + j * sub_cols, sub_cols), sub_cols)

    def attend(b, n, half):
        q = q_buf[n]
        row = b * rb + lax.rem(lax.broadcasted_iota(jnp.int32, (2 * rb, 1), 0), rb) + jnp.where(last, 0, keys)
        first, width = half * (keys // 2), keys // 2
        scores = lax.dot_general(q, k_buf[n, first:first + width, :], (((1,), (1,)), ((), ())), preferred_element_type=F32)
        parts = []
        for start in range(0, width, chunk_keys):
            s, key = scores[:, start:start + chunk_keys], first + start
            if key >= keys - chunk_len:
                column = key - (keys - chunk_len) + lax.broadcasted_iota(jnp.int32, (1, chunk_keys), 1)
                s = jnp.where(column <= row, s, -jnp.inf)
            elif key > 0:
                s = s + bias_ref[0:1, key:key + chunk_keys]
            parts.append(s)
        m = jnp.max(functools.reduce(jnp.maximum, parts), axis=-1, keepdims=True)
        if half:
            m = jnp.maximum(m, att_m[...])
        weights = [jnp.exp2((s - m) * scale) for s in parts]
        l = jnp.sum(functools.reduce(jnp.add, weights), axis=-1, keepdims=True)
        acc = jnp.dot(jnp.concatenate([p.astype(BF16) for p in weights], axis=1), v_buf[n, first:first + width, :], preferred_element_type=F32)
        if half:
            fade = jnp.exp2((att_m[...] - m) * scale)
            l, acc = att_l[...] * fade + l, att_acc[...] * fade + acc
        if not half:
            att_m[...], att_l[...], att_acc[...] = m, l, acc
        return acc, m, l

    def stage_attend(b, piece):
        head, half = piece // 2, piece % 2
        n = c if head else other_c

        if piece == 0:
            project_q(b)
        if head == 0:
            @pl.when(b == 0)
            def _():
                prepare_keys(half)

        acc, m, l = attend(b, n, half)
        if not half:
            return
        tile = stats_tile(rb, [m[:rb], l[:rb], m[rb:], l[rb:]])
        if head:
            own_num[:, 0:128] = acc[:rb]
            own_num[:, 128:256] = acc[rb:]
            own_st[...] = tile
        else:
            a_send[b, :rb, 0:128] = acc[:rb]
            a_send[b, :rb, 128:256] = acc[rb:]
            rows8 = stats_rows(tile)
            a_send[b, rb:rb + STAT_ROWS, :] = jnp.concatenate([rows8, rows8], axis=1)
            copy_a(b).start()

    def stage_core_merge(b):
        copy_a(b).wait_recv()
        peer_tile = stats_columns(a_recv[b, rb:rb + STAT_ROWS, 0:128])
        nums, columns = merge(own_num[...], own_st[...], a_recv[b, :rb, :], peer_tile, scale)
        tile = stats_tile(rb, columns)
        comb_num[:, 0:128] = nums[0]
        comb_num[:, 128:256] = nums[1]
        comb_st[...] = tile
        mine = pl.ds(pl.multiple_of(y * hb, hb), hb)
        theirs = pl.ds(pl.multiple_of(other_y * hb, hb), hb)
        y_send[b, :hb, :] = comb_num[theirs, :]
        rows8 = stats_rows(tile)
        y_send[b, hb:hb + STAT_ROWS, :] = jnp.concatenate([rows8, rows8], axis=1)
        copy_y(b).start()
        y_num[b] = comb_num[mine, :]
        y_st[b] = comb_st[mine, :]

    def stage_y_merge(b):
        copy_y(b).wait_recv()
        comb_st[...] = stats_columns(y_recv[b, hb:hb + STAT_ROWS, 0:128])
        peer_tile = comb_st[pl.ds(pl.multiple_of(y * hb, hb), hb), :]
        nums, columns = merge(y_num[b], y_st[b], y_recv[b, :hb, :], peer_tile, scale)
        o = jnp.concatenate([nums[0] / columns[1], nums[1] / columns[3]], axis=1).astype(BF16)
        o_send[b] = o.astype(F32)
        copy_o(b).start()
        o_own[b] = o

    def stage_project(b):
        @pl.when(b == 0)
        def _():
            w_load.wait()

        copy_o(b).wait_recv()
        w_mine = w_buf[pl.ds(pl.multiple_of(c * head_cols, head_cols), head_cols), :]
        w_peer = w_buf[pl.ds(pl.multiple_of(other_c * head_cols, head_cols), head_cols), :]
        part = jnp.dot(o_own[b], w_mine, preferred_element_type=F32)
        part = part + jnp.dot(o_recv[b].astype(BF16), w_peer, preferred_element_type=F32)
        for j in range(SUBS):
            p_buf[b, j] = part[:, j * sub_cols:(j + 1) * sub_cols]

        @pl.when(is_end)
        def _():
            for j in range(SUBS):
                copy_p(b, j).start()

    def stage_pair_sum(b, j):
        copy_p(b, j).wait_recv()
        m_send[b, j] = p_buf[b, j] + p_recv[b, j]
        copy_m(b, j).start()

    def stage_total(b, j):
        copy_m(b, j).wait_recv()
        hidden = h_buf[half_rows(b, y), columns_of(c, j)].astype(F32)
        result = (hidden + (m_send[b, j] + m_recv[b, j])).astype(BF16)
        f_buf[b, j] = result.astype(F32)
        copy_f(b, j).start()
        copy_yf(b, j).start()
        copy_d1(b, j).start()
        out_buf[half_rows(b, y), columns_of(c, j)] = result

    def stage_end_total(b, j):
        copy_f(b, j).wait_recv()
        copy_yf(b, j).start()
        copy_d1(b, j).start()
        out_buf[half_rows(b, y), columns_of(c, j)] = f_buf[b, j].astype(BF16)

    def stage_y_total(b, j):
        copy_yf(b, j).wait_recv()
        copy_d2(b, j).start()
        out_buf[half_rows(b, other_y), columns_of(c, j)] = yf_recv[b, j].astype(BF16)

    def stage_store(b, j):
        copy_d1(b, j).wait_recv()
        out_buf[half_rows(b, y), columns_of(other_c, j)] = d1_recv[b, j].astype(BF16)
        copy_d2(b, j).wait_recv()
        out_buf[half_rows(b, other_y), columns_of(other_c, j)] = d2_recv[b, j].astype(BF16)
        if j == SUBS - 1:
            out_store(b).start()

    def stage_sent(b):
        for sent in (copy_a, copy_y, copy_o):
            sent(b).wait_send()
        out_store(b).wait()
        for j in range(SUBS):
            for sent in (copy_yf, copy_d1, copy_d2):
                sent(b, j).wait_send()

        @pl.when(is_mid)
        def _():
            for j in range(SUBS):
                copy_m(b, j).wait_send()
                copy_f(b, j).wait_send()

        @pl.when(is_end)
        def _():
            for j in range(SUBS):
                copy_p(b, j).wait_send()

    def run(stage, it, step, lag, guard=None, sub=True):
        j = (step - lag) % SUBS
        if not sub and j:
            return
        b = it + (step - lag - j) // SUBS
        live = jnp.logical_and(b >= 0, b < nb)
        if guard is not None:
            live = jnp.logical_and(live, guard)

        @pl.when(live)
        def _():
            if sub:
                stage(b, j)
            else:
                stage(b)

    lag_p, hop = LAG_PROJECT + LAG_HOP, LAG_HOP
    lag_store = lag_p + 3 * hop + 2

    def body(it, carry):
        for step in range(SUBS):
            run(stage_store, it, step, lag_store)
            run(stage_y_total, it, step, lag_p + 3 * hop, is_end)
            run(stage_end_total, it, step, lag_p + 2 * hop, is_end)
            run(stage_y_total, it, step, lag_p + 2 * hop, is_mid)
            run(stage_total, it, step, lag_p + hop, is_mid)
            run(stage_pair_sum, it, step, lag_p, is_mid)
            run(stage_attend, it, step, 0)
            run(stage_core_merge, it, step, SUBS - 1, sub=False)
            run(stage_y_merge, it, step, LAG_Y, sub=False)
            run(stage_project, it, step, LAG_PROJECT, sub=False)
        return carry

    lax.fori_loop(0, nb + (lag_store + SUBS - 1) // SUBS, body, 0)
    lax.fori_loop(0, nb, lambda b, carry: (stage_sent(b), carry)[1], 0)

    @pl.when(last)
    def _():
        kn_store.wait()
        vn_store.wait()


def finish_kernel(cfg, pos_ref, kc_hbm, vc_hbm, kn_hbm, vn_hbm, x_hbm, kc_out, vc_out, x_out, kc_buf, vc_buf, kn_buf, vn_buf, x_buf, in_sems, out_sems):
    last_index, parts = cfg
    is_last = lax.axis_index("sp") == last_index
    shard_len, chunk_len = kc_buf.shape[0], kn_buf.shape[0]
    write_at = jnp.clip(pos_ref[0] - last_index * shard_len, 0, shard_len - chunk_len)
    jobs = []
    for src, buf, dst in ((kc_hbm, kc_buf, kc_out), (vc_hbm, vc_buf, vc_out), (x_hbm, x_buf, x_out)):
        rows = buf.shape[0] // parts
        for part in range(parts):
            span = pl.ds(part * rows, rows)
            k = len(jobs)
            jobs.append((pltpu.make_async_copy(src.at[span], buf.at[span], in_sems.at[k]), pltpu.make_async_copy(buf.at[span], dst.at[span], out_sems.at[k])))
    k = len(jobs)
    new_loads = [pltpu.make_async_copy(kn_hbm, kn_buf, in_sems.at[k]), pltpu.make_async_copy(vn_hbm, vn_buf, in_sems.at[k + 1])]
    new_stores = [pltpu.make_async_copy(kn_buf, kc_out.at[pl.ds(write_at, chunk_len)], out_sems.at[k]),
                  pltpu.make_async_copy(vn_buf, vc_out.at[pl.ds(write_at, chunk_len)], out_sems.at[k + 1])]
    for load, _ in jobs[:2 * parts]:
        load.start()

    @pl.when(is_last)
    def _():
        for load in new_loads:
            load.start()

    for load, _ in jobs[2 * parts:]:
        load.start()
    for load, store in jobs:
        load.wait()
        store.start()
    for _, store in jobs[:2 * parts]:
        store.wait()

    @pl.when(is_last)
    def _():
        for load, store in zip(new_loads, new_stores):
            load.wait()
            store.start()
        for store in new_stores:
            store.wait()

    for _, store in jobs[2 * parts:]:
        store.wait()


def finish_call(start_pos, k_shard, v_shard, k_new, v_new, result, last_index, parts=4):
    hbm = pl.BlockSpec(memory_space=pl.ANY)
    shapes = [jax.ShapeDtypeStruct(x.shape, x.dtype) for x in (k_shard, v_shard, result)]
    return pl.pallas_call(
        functools.partial(finish_kernel, (last_index, parts)),
        out_shape=tuple(shapes),
        in_specs=[pl.BlockSpec(memory_space=pltpu.SMEM)] + [hbm] * 5,
        out_specs=(hbm, hbm, hbm),
        scratch_shapes=[pltpu.VMEM(x.shape, x.dtype) for x in (k_shard, v_shard, k_new, v_new, result)]
        + [pltpu.SemaphoreType.DMA((3 * parts + 2,)), pltpu.SemaphoreType.DMA((3 * parts + 2,))],
        compiler_params=pltpu.CompilerParams(vmem_limit_bytes=60 * 2**20),
        name="finish",
    )(start_pos, k_shard, v_shard, k_new, v_new, result)


def attend_call(start_pos, hidden, norm_gain, w_query, w_key, w_value, q_gain, k_gain, cosine, sine, k_shard, v_shard, w_out, chunk_keys, scale, z_count):
    chunk_len, model_dim = hidden.shape
    keys, kv_local, head_dim = k_shard.shape
    rb = ROW_BLOCK
    nb, hb = chunk_len // rb, rb // 2
    half_cols = model_dim // 2
    heads = w_out.shape[0] // 2
    cfg = (nb, rb, keys, chunk_keys, chunk_len, scale, z_count)
    sub = pltpu.VMEM((nb, SUBS, hb, half_cols // SUBS), F32)
    flops = 4 * 4 * chunk_len * keys * 128 + 2 * chunk_len * w_out.shape[0] * model_dim // 4
    vmem = pl.BlockSpec(memory_space=pltpu.VMEM)
    hbm = pl.BlockSpec(memory_space=pl.ANY)
    new_shape = jax.ShapeDtypeStruct((chunk_len, kv_local, head_dim), BF16)
    return pl.pallas_call(
        functools.partial(attend_kernel, cfg),
        out_shape=(jax.ShapeDtypeStruct((chunk_len, model_dim), BF16), new_shape, new_shape),
        in_specs=[pl.BlockSpec(memory_space=pltpu.SMEM), hbm, vmem, hbm, hbm, hbm, vmem, vmem, vmem, vmem, hbm, hbm, hbm],
        out_specs=(hbm, hbm, hbm),
        scratch_shapes=[
            pltpu.VMEM((chunk_len, model_dim), BF16),
            pltpu.VMEM(w_query.shape, BF16),
            pltpu.VMEM((model_dim, 2 * w_key.shape[1]), BF16),
            pltpu.VMEM(k_shard.shape, BF16),
            pltpu.VMEM(k_shard.shape, BF16),
            pltpu.VMEM((kv_local, keys, head_dim), BF16),
            pltpu.VMEM((kv_local, keys, head_dim), BF16),
            pltpu.VMEM((2, chunk_len, kv_local, head_dim), BF16),
            pltpu.VMEM((kv_local, 2 * rb, head_dim), BF16),
            pltpu.VMEM((1, keys), F32),
            pltpu.VMEM((w_out.shape[0], half_cols), BF16),
            pltpu.VMEM((chunk_len, model_dim), BF16),
            pltpu.VMEM((2 * rb, 1), F32),
            pltpu.VMEM((2 * rb, 1), F32),
            pltpu.VMEM((2 * rb, 128), F32),
            pltpu.VMEM((nb, rb + STAT_ROWS, heads), F32),
            pltpu.VMEM((nb, rb + STAT_ROWS, heads), F32),
            pltpu.VMEM((rb, heads), F32),
            pltpu.VMEM((rb, 128), F32),
            pltpu.VMEM((rb, heads), F32),
            pltpu.VMEM((rb, 128), F32),
            pltpu.VMEM((nb, hb + STAT_ROWS, heads), F32),
            pltpu.VMEM((nb, hb + STAT_ROWS, heads), F32),
            pltpu.VMEM((nb, hb, heads), F32),
            pltpu.VMEM((nb, hb, 128), F32),
            pltpu.VMEM((nb, hb, heads), BF16),
            pltpu.VMEM((nb, hb, heads), F32),
            pltpu.VMEM((nb, hb, heads), F32),
            sub, sub, sub, sub, sub, sub, sub, sub,
            pltpu.SemaphoreType.DMA((3, nb)),
            pltpu.SemaphoreType.DMA((3, nb)),
            pltpu.SemaphoreType.DMA((6, nb, SUBS)),
            pltpu.SemaphoreType.DMA((6, nb, SUBS)),
            pltpu.SemaphoreType.DMA((2, 2)),
            pltpu.SemaphoreType.DMA((4,)),
            pltpu.SemaphoreType.DMA((nb,)),
            pltpu.SemaphoreType.DMA((2,)),
            pltpu.SemaphoreType.DMA((nb,)),
        ],
        compiler_params=pltpu.CompilerParams(collective_id=0, has_side_effects=True, vmem_limit_bytes=62 * 2**20),
        cost_estimate=pl.CostEstimate(flops=flops, bytes_accessed=16 * 2**20, transcendentals=4 * chunk_len * keys),
        name="attend",
    )(start_pos, hidden, norm_gain[None, :], w_query, w_key, w_value, q_gain[None, :], k_gain[None, :], cosine, sine, k_shard, v_shard, w_out)


def solution(mesh, chunk_keys=1024):
    cache_spec = P(("dp", "sp"), "tp", None)
    in_specs = (P("dp", None), P("dp"), cache_spec, cache_spec, P(None), P(None, "tp"), P(None, "tp"), P(None, "tp"), P(None), P(None), P("tp", None))
    out_specs = (P("dp", None), cache_spec, cache_spec)

    def local_step(hidden, start_pos, k_shard, v_shard, norm_gain, w_query, w_key, w_value, q_gain, k_gain, w_out):
        chunk_len, model_dim = hidden.shape
        shard_len, kv_local, head_dim = k_shard.shape
        positions = start_pos[0] + jnp.arange(chunk_len, dtype=jnp.int32)
        cosine, sine = rotary_tables(positions, head_dim)
        scale = LOG2E * head_dim ** -0.5
        result, k_new, v_new = attend_call(start_pos, hidden, norm_gain, w_query, w_key, w_value, q_gain, k_gain, cosine, sine, k_shard, v_shard, w_out,
                                           chunk_keys, scale, mesh.shape["tp"])
        k_upd, v_upd, out = finish_call(start_pos, k_shard, v_shard, k_new, v_new, result, LAST_SHARD)
        return out, k_upd, v_upd

    return jax.shard_map(local_step, mesh=mesh, in_specs=in_specs, out_specs=out_specs, check_vma=False)
```

```python
import functools

import jax
import jax.numpy as jnp
from jax import lax
from jax.experimental import pallas as pl
from jax.experimental.pallas import tpu as pltpu
from jax.sharding import PartitionSpec as P

ROPE_BASE = 1e6
NORM_EPS = 1e-6
LOG2E = 1.4426950408889634
MESH = pl.DeviceIdType.MESH
F32 = jnp.float32
BF16 = jnp.bfloat16
ROW_BLOCK = 128
STAT_ROWS = 8
SUBS = 4
PIECE_STEPS = SUBS // 4
LAG_Y = 6
LAG_PROJECT = 7
LAG_P = 3
LAG_M = 3
LAG_F = 3
LAG_YF = 3
LAST_SHARD = 3
ATTEND_VMEM = 50


def rotary_tables(first_pos, chunk_len, head_dim):
    half_dim = head_dim // 2
    inv_freq = ROPE_BASE ** (-2.0 * jnp.arange(half_dim, dtype=jnp.float32) / head_dim)
    starts = first_pos + ROW_BLOCK * jnp.arange(chunk_len // ROW_BLOCK, dtype=jnp.int32)
    places = jnp.concatenate([starts, jnp.arange(ROW_BLOCK, dtype=jnp.int32)])
    angles = places.astype(jnp.float32)[:, None] * jnp.tile(inv_freq, 2)[None, :]
    return jnp.cos(angles), jnp.sin(angles)


def stats_tile(rows, columns):
    lane = lax.broadcasted_iota(jnp.int32, (rows, 128), 1)
    tile = jnp.zeros((rows, 128), F32)
    for k, column in enumerate(columns):
        tile = jnp.where(lane == k, column, tile)
    return tile


def stats_rows(tile):
    return jnp.transpose(tile)[:STAT_ROWS]


def stats_columns(rows8):
    return jnp.transpose(jnp.concatenate([rows8] * (128 // STAT_ROWS), axis=0))


def merge(num_a, tile_a, num_b, tile_b, scale):
    nums, columns = [], []
    for g in range(2):
        m_a, l_a = tile_a[:, 2 * g:2 * g + 1], tile_a[:, 2 * g + 1:2 * g + 2]
        m_b, l_b = tile_b[:, 2 * g:2 * g + 1], tile_b[:, 2 * g + 1:2 * g + 2]
        m = jnp.maximum(m_a, m_b)
        c_a = jnp.exp2((m_a - m) * scale)
        c_b = jnp.exp2((m_b - m) * scale)
        nums.append(num_a[:, g * 128:(g + 1) * 128] * c_a + num_b[:, g * 128:(g + 1) * 128] * c_b)
        columns += [m, l_a * c_a + l_b * c_b]
    return nums, columns


def attend_kernel(cfg, pos_ref, h_hbm, gain_ref, wq_hbm, wk_hbm, wv_hbm, qg_ref, kg_ref, cos_ref, sin_ref, kc_hbm, vc_hbm, w_hbm, out_buf, kc_buf, vc_buf, new_buf,
                  h_buf, wq_buf, wkv_buf, k_buf, v_buf, q_buf, bias_ref, w_buf, att_m, att_l, att_acc,
                  a_send, a_recv, own_num, own_st, comb_num, comb_st, y_send, y_recv, y_num, y_st, o_own, o_send, o_recv,
                  p_buf, p_recv, m_send, m_recv, f_buf, yf_recv, d1_recv, d2_recv, row_send, row_recv, sub_send, sub_recv,
                  kv_sems, w_sems, h_sems):
    nb, rb, keys, chunk_keys, chunk_len, scale, z_count = cfg
    hb = rb // 2
    dp, z, sp = lax.axis_index("dp"), lax.axis_index("tp"), lax.axis_index("sp")
    y, c = lax.div(sp, 2), lax.rem(sp, 2)
    other_y, other_c = 1 - y, 1 - c
    pair_z = z + 1 - 2 * lax.rem(z, 2)
    cross_z = z_count - 1 - z
    is_mid = jnp.logical_and(z >= 1, z <= 2)
    is_end = jnp.logical_not(is_mid)
    half_cols = w_buf.shape[1]
    sub_cols = half_cols // SUBS
    head_cols = w_buf.shape[0] // 2
    core_peer = (dp, z, y * 2 + other_c)
    y_peer = (dp, z, other_y * 2 + c)
    pair_peer = (dp, pair_z, sp)
    cross_peer = (dp, cross_z, sp)
    my_cols = pl.ds(pl.multiple_of(c * half_cols, half_cols), half_cols)

    last = sp == LAST_SHARD
    old_len = keys - chunk_len
    kv_cols = wk_hbm.shape[1]
    limit = jnp.where(last, pos_ref[0] - LAST_SHARD * keys, keys)

    def half_rows(b, which):
        return pl.ds(pl.multiple_of(b * rb + which * hb, hb), hb)

    def block_rows(b, rows):
        return pl.ds(pl.multiple_of(b * rows, rows), rows)

    def cache_loads(half):
        span = pl.ds(half * (keys // 2), keys // 2)
        return (pltpu.make_async_copy(kc_hbm.at[span], kc_buf.at[span], kv_sems.at[0, half]),
                pltpu.make_async_copy(vc_hbm.at[span], vc_buf.at[span], kv_sems.at[1, half]))

    def h_load(b):
        return pltpu.make_async_copy(h_hbm.at[block_rows(b, rb)], h_buf.at[block_rows(b, rb)], h_sems.at[b])

    wq_load = pltpu.make_async_copy(wq_hbm, wq_buf, w_sems.at[0])
    wk_load = pltpu.make_async_copy(wk_hbm, wkv_buf.at[:, pl.ds(0, kv_cols)], w_sems.at[1])
    wv_load = pltpu.make_async_copy(wv_hbm, wkv_buf.at[:, pl.ds(kv_cols, kv_cols)], w_sems.at[2])
    w_load = pltpu.make_async_copy(w_hbm.at[:, my_cols], w_buf, w_sems.at[3])

    @pl.when(last)
    def _():
        wk_load.start()
        wv_load.start()

    h_load(0).start()
    h_load(1).start()
    wq_load.start()
    for half in range(2):
        for load in cache_loads(half):
            load.start()
    for b in range(2, nb):
        h_load(b).start()
    w_load.start()

    barrier = pltpu.get_barrier_semaphore()
    for peer in (core_peer, y_peer, pair_peer):
        pl.semaphore_signal(barrier, inc=1, device_id=peer, device_id_type=MESH)

    @pl.when(is_mid)
    def _():
        pl.semaphore_signal(barrier, inc=1, device_id=cross_peer, device_id_type=MESH)
        pl.semaphore_wait(barrier, 4)

    @pl.when(is_end)
    def _():
        pl.semaphore_wait(barrier, 3)

    key_index = lax.broadcasted_iota(jnp.int32, (1, keys), 1)
    bias_ref[...] = jnp.where(key_index < limit, 0.0, -jnp.inf).astype(F32)

    def normalize(x, gain):
        return x * lax.rsqrt(jnp.mean(x * x, axis=-1, keepdims=True) + NORM_EPS) * gain

    def block_angles(b):
        cos_a, sin_a = cos_ref[pl.ds(b, 1), :], sin_ref[pl.ds(b, 1), :]
        cos_b, sin_b = cos_ref[nb:nb + rb, :], sin_ref[nb:nb + rb, :]
        lane = lax.broadcasted_iota(jnp.int32, (rb, 128), 1)
        sine = sin_a * cos_b + cos_a * sin_b
        return cos_a * cos_b - sin_a * sin_b, jnp.where(lane < 64, -sine, sine)

    def rotate(x, angles):
        return (x * angles[0] + pltpu.roll(x, 64, 1) * angles[1]).astype(BF16)

    def project_q(b):
        @pl.when(jnp.logical_not(last))
        def _():
            h_load(b).wait()

        @pl.when(b == 0)
        def _():
            wq_load.wait()

        span = block_rows(b, rb)
        normed = normalize(h_buf[span, :].astype(F32), gain_ref[...]).astype(BF16)
        proj = jnp.dot(normed, wq_buf[...], preferred_element_type=F32)
        angles = block_angles(b)
        for head in range(4):
            q_buf[head // 2, (head % 2) * rb:(head % 2 + 1) * rb, :] = rotate(normalize(proj[:, head * 128:(head + 1) * 128], qg_ref[...]), angles)

    def project_new(part):
        rows = 2 * rb
        for b in range(2):
            h_load(2 * part + b).wait()
        span = block_rows(part, rows)
        normed = normalize(h_buf[span, :].astype(F32), gain_ref[...]).astype(BF16)
        proj = jnp.dot(normed, wkv_buf[...], preferred_element_type=F32)
        angles = [jnp.concatenate(pair, axis=0) for pair in zip(block_angles(2 * part), block_angles(2 * part + 1))]
        place = pl.ds(pl.multiple_of(old_len + part * rows, rows), rows)
        heads = []
        for n in range(2):
            heads.append(rotate(normalize(proj[:, n * 128:(n + 1) * 128], kg_ref[...]), angles))
            k_buf[n, place, :] = heads[n]
            v_buf[n, place, :] = proj[:, kv_cols + n * 128:kv_cols + (n + 1) * 128].astype(BF16)
        new_buf[0, span] = jnp.concatenate(heads, axis=1).reshape(rows, 2, 128)
        new_buf[1, span] = proj[:, kv_cols:].astype(BF16).reshape(rows, 2, 128)

    def split_heads(start, stop):
        for src, dst in ((kc_buf, k_buf), (vc_buf, v_buf)):
            for row in range(start, stop, 256):
                x = src[row:row + 256].reshape(256, kv_cols)
                for n in range(2):
                    dst[n, row:row + 256, :] = x[:, n * 128:(n + 1) * 128]

    def prepare_keys(half):
        for load in cache_loads(half):
            load.wait()
        if half == 0:
            split_heads(0, keys // 2)
        else:
            split_heads(keys // 2, old_len)

            @pl.when(jnp.logical_not(last))
            def _():
                split_heads(old_len, keys)

    @pl.when(last)
    def _():
        wk_load.wait()
        wv_load.wait()
        for n in range(2):
            k_buf[n, old_len:keys, :] = jnp.zeros((chunk_len, 128), BF16)
            v_buf[n, old_len:keys, :] = jnp.zeros((chunk_len, 128), BF16)

    def row_copy(kind, b, src, dst, peer):
        return pltpu.make_async_remote_copy(src.at[b], dst.at[b], row_send.at[kind, b], row_recv.at[kind, b], device_id=peer, device_id_type=MESH)

    def sub_copy(kind, b, j, src, dst, peer):
        return pltpu.make_async_remote_copy(src.at[b, j], dst.at[b, j], sub_send.at[kind, b], sub_recv.at[kind, b, j], device_id=peer, device_id_type=MESH)

    copy_a = lambda b: row_copy(0, b, a_send, a_recv, core_peer)
    copy_y = lambda b: row_copy(1, b, y_send, y_recv, y_peer)
    copy_o = lambda b: row_copy(2, b, o_send, o_recv, core_peer)
    copy_p = lambda b, j: sub_copy(0, b, j, p_buf, p_recv, pair_peer)
    copy_m = lambda b, j: sub_copy(1, b, j, m_send, m_recv, cross_peer)
    copy_f = lambda b, j: sub_copy(2, b, j, f_buf, f_buf, pair_peer)
    copy_yf = lambda b, j: sub_copy(3, b, j, f_buf, yf_recv, y_peer)
    copy_d1 = lambda b, j: sub_copy(4, b, j, f_buf, d1_recv, core_peer)
    copy_d2 = lambda b, j: sub_copy(5, b, j, yf_recv, d2_recv, core_peer)

    def sub_sent(kind, b, src, dst, peer):
        pltpu.make_async_remote_copy(src.at[b], dst.at[b], sub_send.at[kind, b], sub_recv.at[kind, b, 0], device_id=peer, device_id_type=MESH).wait_send()

    def columns_of(core, j):
        return pl.ds(pl.multiple_of(core * half_cols + j * sub_cols, sub_cols), sub_cols)

    def attend(b, n, half):
        q = q_buf[n]
        row = b * rb + lax.rem(lax.broadcasted_iota(jnp.int32, (2 * rb, 1), 0), rb) + jnp.where(last, 0, keys)
        first, width = half * (keys // 2), keys // 2
        scores = lax.dot_general(q, k_buf[n, first:first + width, :], (((1,), (1,)), ((), ())), preferred_element_type=F32)
        parts = []
        for start in range(0, width, chunk_keys):
            s, key = scores[:, start:start + chunk_keys], first + start
            if key >= keys - chunk_len:
                column = key - (keys - chunk_len) + lax.broadcasted_iota(jnp.int32, (1, chunk_keys), 1)
                s = jnp.where(column <= row, s, -jnp.inf)
            elif key > 0:
                s = s + bias_ref[0:1, key:key + chunk_keys]
            parts.append(s)
        m = jnp.max(functools.reduce(jnp.maximum, parts), axis=-1, keepdims=True)
        if half:
            m = jnp.maximum(m, att_m[...])
        weights = [jnp.exp2((s - m) * scale) for s in parts]
        l = jnp.sum(functools.reduce(jnp.add, weights), axis=-1, keepdims=True)
        acc = jnp.dot(jnp.concatenate([p.astype(BF16) for p in weights], axis=1), v_buf[n, first:first + width, :], preferred_element_type=F32)
        if half:
            fade = jnp.exp2((att_m[...] - m) * scale)
            l, acc = att_l[...] * fade + l, att_acc[...] * fade + acc
        if not half:
            att_m[...], att_l[...], att_acc[...] = m, l, acc
        return acc, m, l

    def stage_attend(b, piece):
        head, half = piece // 2, piece % 2
        n = c if head else other_c

        if piece == 0:
            @pl.when(jnp.logical_and(last, lax.rem(b, 2) == 0))
            def _():
                project_new(lax.div(b, 2))

            project_q(b)
        if head == 0:
            @pl.when(b == 0)
            def _():
                prepare_keys(half)

        acc, m, l = attend(b, n, half)
        if not half:
            return
        tile = stats_tile(rb, [m[:rb], l[:rb], m[rb:], l[rb:]])
        if head:
            own_num[:, 0:128] = acc[:rb]
            own_num[:, 128:256] = acc[rb:]
            own_st[...] = tile
        else:
            a_send[b, :rb, 0:128] = acc[:rb]
            a_send[b, :rb, 128:256] = acc[rb:]
            rows8 = stats_rows(tile)
            a_send[b, rb:rb + STAT_ROWS, :] = jnp.concatenate([rows8, rows8], axis=1)
            copy_a(b).start()

    def stage_core_merge(b):
        copy_a(b).wait_recv()
        peer_tile = stats_columns(a_recv[b, rb:rb + STAT_ROWS, 0:128])
        nums, columns = merge(own_num[...], own_st[...], a_recv[b, :rb, :], peer_tile, scale)
        tile = stats_tile(rb, columns)
        comb_num[:, 0:128] = nums[0]
        comb_num[:, 128:256] = nums[1]
        comb_st[...] = tile
        mine = pl.ds(pl.multiple_of(y * hb, hb), hb)
        theirs = pl.ds(pl.multiple_of(other_y * hb, hb), hb)
        y_send[b, :hb, :] = comb_num[theirs, :]
        rows8 = stats_rows(tile)
        y_send[b, hb:hb + STAT_ROWS, :] = jnp.concatenate([rows8, rows8], axis=1)
        copy_y(b).start()
        y_num[b] = comb_num[mine, :]
        y_st[b] = comb_st[mine, :]

    def stage_y_merge(b):
        copy_y(b).wait_recv()
        comb_st[...] = stats_columns(y_recv[b, hb:hb + STAT_ROWS, 0:128])
        peer_tile = comb_st[pl.ds(pl.multiple_of(y * hb, hb), hb), :]
        nums, columns = merge(y_num[b], y_st[b], y_recv[b, :hb, :], peer_tile, scale)
        o = jnp.concatenate([nums[0] / columns[1], nums[1] / columns[3]], axis=1).astype(BF16)
        o_send[b] = o.astype(F32)
        copy_o(b).start()
        o_own[b] = o

    def stage_project(b):
        @pl.when(b == 0)
        def _():
            w_load.wait()

        copy_o(b).wait_recv()
        w_mine = w_buf[pl.ds(pl.multiple_of(c * head_cols, head_cols), head_cols), :]
        w_peer = w_buf[pl.ds(pl.multiple_of(other_c * head_cols, head_cols), head_cols), :]
        part = jnp.dot(o_own[b], w_mine, preferred_element_type=F32)
        part = part + jnp.dot(o_recv[b].astype(BF16), w_peer, preferred_element_type=F32)
        for j in range(SUBS):
            p_buf[b, j] = part[:, j * sub_cols:(j + 1) * sub_cols]

        @pl.when(is_end)
        def _():
            for j in range(SUBS):
                copy_p(b, j).start()

    def stage_pair_sum(b, j):
        copy_p(b, j).wait_recv()
        m_send[b, j] = p_buf[b, j] + p_recv[b, j]
        copy_m(b, j).start()

    def stage_total(b, j):
        copy_m(b, j).wait_recv()
        hidden = h_buf[half_rows(b, y), columns_of(c, j)].astype(F32)
        result = (hidden + (m_send[b, j] + m_recv[b, j])).astype(BF16)
        f_buf[b, j] = result.astype(F32)
        copy_f(b, j).start()
        copy_yf(b, j).start()
        copy_d1(b, j).start()
        out_buf[half_rows(b, y), columns_of(c, j)] = result

    def stage_end_total(b, j):
        copy_f(b, j).wait_recv()
        copy_yf(b, j).start()
        copy_d1(b, j).start()
        out_buf[half_rows(b, y), columns_of(c, j)] = f_buf[b, j].astype(BF16)

    def stage_y_total(b, j):
        copy_yf(b, j).wait_recv()
        copy_d2(b, j).start()
        out_buf[half_rows(b, other_y), columns_of(c, j)] = yf_recv[b, j].astype(BF16)

    def stage_store(b, j):
        copy_d1(b, j).wait_recv()
        out_buf[half_rows(b, y), columns_of(other_c, j)] = d1_recv[b, j].astype(BF16)
        copy_d2(b, j).wait_recv()
        out_buf[half_rows(b, other_y), columns_of(other_c, j)] = d2_recv[b, j].astype(BF16)

    def stage_sent(b):
        for sent in (copy_a, copy_y, copy_o):
            sent(b).wait_send()
        sub_sent(3, b, f_buf, yf_recv, y_peer)
        sub_sent(4, b, f_buf, d1_recv, core_peer)
        sub_sent(5, b, yf_recv, d2_recv, core_peer)

        @pl.when(is_mid)
        def _():
            sub_sent(1, b, m_send, m_recv, cross_peer)
            sub_sent(2, b, f_buf, f_buf, pair_peer)

        @pl.when(is_end)
        def _():
            sub_sent(0, b, p_buf, p_recv, pair_peer)

    def run(stage, it, step, lag, guard=None, sub=True):
        j = (step - lag) % SUBS
        if not sub and j:
            return
        b = it + (step - lag - j) // SUBS
        live = jnp.logical_and(b >= 0, b < nb)
        if guard is not None:
            live = jnp.logical_and(live, guard)

        @pl.when(live)
        def _():
            if sub:
                stage(b, j)
            else:
                stage(b)

    lag_p = LAG_PROJECT + LAG_P
    lag_m = lag_p + LAG_M
    lag_f = lag_m + LAG_F
    lag_store = lag_f + LAG_YF + 2

    def body(it, carry):
        for step in range(SUBS):
            run(stage_store, it, step, lag_store)
            run(stage_y_total, it, step, lag_f + LAG_YF, is_end)
            run(stage_end_total, it, step, lag_f, is_end)
            run(stage_y_total, it, step, lag_m + LAG_YF, is_mid)
            run(stage_total, it, step, lag_m, is_mid)
            run(stage_pair_sum, it, step, lag_p, is_mid)
            if step % PIECE_STEPS == 0:
                run(lambda b, j: stage_attend(b, j // PIECE_STEPS), it, step, 0)
            run(stage_core_merge, it, step, 3 * PIECE_STEPS, sub=False)
            run(stage_y_merge, it, step, LAG_Y, sub=False)
            run(stage_project, it, step, LAG_PROJECT, sub=False)
        return carry

    lax.fori_loop(0, nb + (lag_store + SUBS - 1) // SUBS, body, 0)
    lax.fori_loop(0, nb, lambda b, carry: (stage_sent(b), carry)[1], 0)


def finish_kernel(pos_ref, kc_buf, vc_buf, new_buf, x_buf, kc_out, vc_out, x_out, sems):
    is_last = lax.axis_index("sp") == LAST_SHARD
    shard_len, chunk_len = kc_buf.shape[0], new_buf.shape[1]
    write_at = jnp.clip(pos_ref[0] - LAST_SHARD * shard_len, 0, shard_len - chunk_len)
    span = pl.ds(write_at, chunk_len)
    k_store = pltpu.make_async_copy(kc_buf, kc_out, sems.at[0])
    v_store = pltpu.make_async_copy(vc_buf, vc_out, sems.at[1])
    x_store = pltpu.make_async_copy(x_buf, x_out, sems.at[2])
    new_stores = (pltpu.make_async_copy(new_buf.at[0], kc_out.at[span], sems.at[3]), pltpu.make_async_copy(new_buf.at[1], vc_out.at[span], sems.at[4]))
    k_store.start()
    v_store.start()
    x_store.start()
    k_store.wait()
    v_store.wait()

    @pl.when(is_last)
    def _():
        for store in new_stores:
            store.start()
        for store in new_stores:
            store.wait()

    x_store.wait()


def finish_call(start_pos, k_old, v_old, new_rows, result):
    hbm = pl.BlockSpec(memory_space=pl.ANY)
    vmem = pl.BlockSpec(memory_space=pltpu.VMEM)
    shapes = [jax.ShapeDtypeStruct(x.shape, x.dtype) for x in (k_old, v_old, result)]
    return pl.pallas_call(
        finish_kernel,
        out_shape=tuple(shapes),
        in_specs=[pl.BlockSpec(memory_space=pltpu.SMEM)] + [vmem] * 4,
        out_specs=(hbm, hbm, hbm),
        scratch_shapes=[pltpu.SemaphoreType.DMA((5,))],
        compiler_params=pltpu.CompilerParams(vmem_limit_bytes=2 * 2**20),
        name="finish",
    )(start_pos, k_old, v_old, new_rows, result)


def attend_call(start_pos, hidden, norm_gain, w_query, w_key, w_value, q_gain, k_gain, cosine, sine, k_shard, v_shard, w_out, chunk_keys, scale, z_count):
    chunk_len, model_dim = hidden.shape
    keys, kv_local, head_dim = k_shard.shape
    rb = ROW_BLOCK
    nb, hb = chunk_len // rb, rb // 2
    half_cols = model_dim // 2
    heads = w_out.shape[0] // 2
    cfg = (nb, rb, keys, chunk_keys, chunk_len, scale, z_count)
    sub = pltpu.VMEM((nb, SUBS, hb, half_cols // SUBS), F32)
    flops = 4 * 4 * chunk_len * keys * 128 + 2 * chunk_len * w_out.shape[0] * model_dim // 4
    vmem = pl.BlockSpec(memory_space=pltpu.VMEM)
    hbm = pl.BlockSpec(memory_space=pl.ANY)
    outs = (pltpu.VMEM((chunk_len, model_dim), BF16), pltpu.VMEM(k_shard.shape, BF16), pltpu.VMEM(k_shard.shape, BF16),
            pltpu.VMEM((2, chunk_len, kv_local, head_dim), BF16))
    return pl.pallas_call(
        functools.partial(attend_kernel, cfg),
        out_shape=outs,
        in_specs=[pl.BlockSpec(memory_space=pltpu.SMEM), hbm, vmem, hbm, hbm, hbm, vmem, vmem, vmem, vmem, hbm, hbm, hbm],
        out_specs=(vmem, vmem, vmem, vmem),
        scratch_shapes=[
            pltpu.VMEM((chunk_len, model_dim), BF16),
            pltpu.VMEM(w_query.shape, BF16),
            pltpu.VMEM((model_dim, 2 * w_key.shape[1]), BF16),
            pltpu.VMEM((kv_local, keys, head_dim), BF16),
            pltpu.VMEM((kv_local, keys, head_dim), BF16),
            pltpu.VMEM((kv_local, 2 * rb, head_dim), BF16),
            pltpu.VMEM((1, keys), F32),
            pltpu.VMEM((w_out.shape[0], half_cols), BF16),
            pltpu.VMEM((2 * rb, 1), F32),
            pltpu.VMEM((2 * rb, 1), F32),
            pltpu.VMEM((2 * rb, 128), F32),
            pltpu.VMEM((nb, rb + STAT_ROWS, heads), F32),
            pltpu.VMEM((nb, rb + STAT_ROWS, heads), F32),
            pltpu.VMEM((rb, heads), F32),
            pltpu.VMEM((rb, 128), F32),
            pltpu.VMEM((rb, heads), F32),
            pltpu.VMEM((rb, 128), F32),
            pltpu.VMEM((nb, hb + STAT_ROWS, heads), F32),
            pltpu.VMEM((nb, hb + STAT_ROWS, heads), F32),
            pltpu.VMEM((nb, hb, heads), F32),
            pltpu.VMEM((nb, hb, 128), F32),
            pltpu.VMEM((nb, hb, heads), BF16),
            pltpu.VMEM((nb, hb, heads), F32),
            pltpu.VMEM((nb, hb, heads), F32),
            sub, sub, sub, sub, sub, sub, sub, sub,
            pltpu.SemaphoreType.DMA((3, nb)),
            pltpu.SemaphoreType.DMA((3, nb)),
            pltpu.SemaphoreType.DMA((6, nb)),
            pltpu.SemaphoreType.DMA((6, nb, SUBS)),
            pltpu.SemaphoreType.DMA((2, 2)),
            pltpu.SemaphoreType.DMA((4,)),
            pltpu.SemaphoreType.DMA((nb,)),
        ],
        compiler_params=pltpu.CompilerParams(collective_id=0, has_side_effects=True, vmem_limit_bytes=ATTEND_VMEM * 2**20),
        cost_estimate=pl.CostEstimate(flops=flops, bytes_accessed=16 * 2**20, transcendentals=4 * chunk_len * keys),
        name="attend",
    )(start_pos, hidden, norm_gain[None, :], w_query, w_key, w_value, q_gain[None, :], k_gain[None, :], cosine, sine, k_shard, v_shard, w_out)


def solution(mesh, chunk_keys=1024):
    cache_spec = P(("dp", "sp"), "tp", None)
    in_specs = (P("dp", None), P("dp"), cache_spec, cache_spec, P(None), P(None, "tp"), P(None, "tp"), P(None, "tp"), P(None), P(None), P("tp", None))
    out_specs = (P("dp", None), cache_spec, cache_spec)

    def local_step(hidden, start_pos, k_shard, v_shard, norm_gain, w_query, w_key, w_value, q_gain, k_gain, w_out):
        chunk_len, model_dim = hidden.shape
        shard_len, kv_local, head_dim = k_shard.shape
        cosine, sine = rotary_tables(start_pos[0], chunk_len, head_dim)
        scale = LOG2E * head_dim ** -0.5
        result, k_old, v_old, new_rows = attend_call(start_pos, hidden, norm_gain, w_query, w_key, w_value, q_gain, k_gain, cosine, sine, k_shard, v_shard, w_out,
                                           chunk_keys, scale, mesh.shape["tp"])
        k_upd, v_upd, out = finish_call(start_pos, k_old, v_old, new_rows, result)
        return out, k_upd, v_upd

    return jax.shard_map(local_step, mesh=mesh, in_specs=in_specs, out_specs=out_specs, check_vma=False)
```

```python
import functools

import jax
import jax.numpy as jnp
from jax import lax
from jax.experimental import pallas as pl
from jax.experimental.pallas import tpu as pltpu
from jax.sharding import PartitionSpec as P

ROPE_BASE = 1e6
NORM_EPS = 1e-6
LOG2E = 1.4426950408889634
MESH = pl.DeviceIdType.MESH
F32 = jnp.float32
BF16 = jnp.bfloat16
ROW_BLOCK = 128
STAT_ROWS = 8
SUBS = 4
PIECE_STEPS = SUBS // 4
LAG_Y = 6
LAG_PROJECT = 7
LAG_P = 3
LAG_M = 3
LAG_F = 3
LAG_YF = 3
LAST_SHARD = 3
ATTEND_VMEM = 50


def rotary_tables(first_pos, chunk_len, head_dim):
    half_dim = head_dim // 2
    inv_freq = ROPE_BASE ** (-2.0 * jnp.arange(half_dim, dtype=jnp.float32) / head_dim)
    starts = first_pos + ROW_BLOCK * jnp.arange(chunk_len // ROW_BLOCK, dtype=jnp.int32)
    places = jnp.concatenate([starts, jnp.arange(ROW_BLOCK, dtype=jnp.int32)])
    angles = places.astype(jnp.float32)[:, None] * jnp.tile(inv_freq, 2)[None, :]
    return jnp.cos(angles), jnp.sin(angles)


def stats_tile(rows, columns):
    lane = lax.broadcasted_iota(jnp.int32, (rows, 128), 1)
    tile = jnp.zeros((rows, 128), F32)
    for k, column in enumerate(columns):
        tile = jnp.where(lane == k, column, tile)
    return tile


def stats_rows(tile):
    return jnp.transpose(tile)[:STAT_ROWS]


def stats_columns(rows8):
    return jnp.transpose(jnp.concatenate([rows8] * (128 // STAT_ROWS), axis=0))


def merge(num_a, tile_a, num_b, tile_b, scale):
    nums, columns = [], []
    for g in range(2):
        m_a, l_a = tile_a[:, 2 * g:2 * g + 1], tile_a[:, 2 * g + 1:2 * g + 2]
        m_b, l_b = tile_b[:, 2 * g:2 * g + 1], tile_b[:, 2 * g + 1:2 * g + 2]
        m = jnp.maximum(m_a, m_b)
        c_a = jnp.exp2((m_a - m) * scale)
        c_b = jnp.exp2((m_b - m) * scale)
        nums.append(num_a[:, g * 128:(g + 1) * 128] * c_a + num_b[:, g * 128:(g + 1) * 128] * c_b)
        columns += [m, l_a * c_a + l_b * c_b]
    return nums, columns


def attend_kernel(cfg, pos_ref, h_hbm, gain_ref, wq_hbm, wk_hbm, wv_hbm, qg_ref, kg_ref, cos_ref, sin_ref, kc_hbm, vc_hbm, w_hbm, out_buf, kc_buf, vc_buf, new_buf,
                  h_buf, wq_buf, wkv_buf, k_buf, v_buf, q_buf, bias_ref, w_buf, att_m, att_l, att_acc,
                  a_send, a_recv, own_num, own_st, comb_num, comb_st, y_send, y_recv, y_num, y_st, o_own, o_send, o_recv,
                  p_buf, p_recv, m_send, m_recv, f_buf, yf_recv, d1_recv, d2_recv, row_send, row_recv, sub_send, sub_recv,
                  kv_sems, w_sems, h_sems):
    nb, rb, keys, chunk_keys, chunk_len, scale, z_count = cfg
    hb = rb // 2
    dp, z, sp = lax.axis_index("dp"), lax.axis_index("tp"), lax.axis_index("sp")
    y, c = lax.div(sp, 2), lax.rem(sp, 2)
    other_y, other_c = 1 - y, 1 - c
    pair_z = z + 1 - 2 * lax.rem(z, 2)
    cross_z = z_count - 1 - z
    is_mid = jnp.logical_and(z >= 1, z <= 2)
    is_end = jnp.logical_not(is_mid)
    half_cols = w_buf.shape[1]
    sub_cols = half_cols // SUBS
    head_cols = w_buf.shape[0] // 2
    core_peer = (dp, z, y * 2 + other_c)
    y_peer = (dp, z, other_y * 2 + c)
    pair_peer = (dp, pair_z, sp)
    cross_peer = (dp, cross_z, sp)
    my_cols = pl.ds(pl.multiple_of(c * half_cols, half_cols), half_cols)

    last = sp == LAST_SHARD
    old_len = keys - chunk_len
    kv_cols = wk_hbm.shape[1]
    limit = jnp.where(last, pos_ref[0] - LAST_SHARD * keys, keys)

    def half_rows(b, which):
        return pl.ds(pl.multiple_of(b * rb + which * hb, hb), hb)

    def block_rows(b, rows):
        return pl.ds(pl.multiple_of(b * rows, rows), rows)

    def cache_loads(half):
        span = pl.ds(half * (keys // 2), keys // 2)
        return (pltpu.make_async_copy(kc_hbm.at[span], kc_buf.at[span], kv_sems.at[0, half]),
                pltpu.make_async_copy(vc_hbm.at[span], vc_buf.at[span], kv_sems.at[1, half]))

    def h_load(b):
        return pltpu.make_async_copy(h_hbm.at[block_rows(b, rb)], h_buf.at[block_rows(b, rb)], h_sems.at[b])

    wq_load = pltpu.make_async_copy(wq_hbm, wq_buf, w_sems.at[0])
    wk_load = pltpu.make_async_copy(wk_hbm, wkv_buf.at[:, pl.ds(0, kv_cols)], w_sems.at[1])
    wv_load = pltpu.make_async_copy(wv_hbm, wkv_buf.at[:, pl.ds(kv_cols, kv_cols)], w_sems.at[2])
    w_load = pltpu.make_async_copy(w_hbm.at[:, my_cols], w_buf, w_sems.at[3])

    @pl.when(last)
    def _():
        wk_load.start()
        wv_load.start()

    h_load(0).start()
    h_load(1).start()
    wq_load.start()
    for half in range(2):
        for load in cache_loads(half):
            load.start()
    for b in range(2, nb):
        h_load(b).start()
    w_load.start()

    barrier = pltpu.get_barrier_semaphore()
    for peer in (core_peer, y_peer, pair_peer):
        pl.semaphore_signal(barrier, inc=1, device_id=peer, device_id_type=MESH)

    @pl.when(is_mid)
    def _():
        pl.semaphore_signal(barrier, inc=1, device_id=cross_peer, device_id_type=MESH)
        pl.semaphore_wait(barrier, 4)

    @pl.when(is_end)
    def _():
        pl.semaphore_wait(barrier, 3)

    key_index = lax.broadcasted_iota(jnp.int32, (1, keys), 1)
    bias_ref[...] = jnp.where(key_index < limit, 0.0, -jnp.inf).astype(F32)

    def normalize(x, gain):
        return x * lax.rsqrt(jnp.mean(x * x, axis=-1, keepdims=True) + NORM_EPS) * gain

    def block_angles(b):
        cos_a, sin_a = cos_ref[pl.ds(b, 1), :], sin_ref[pl.ds(b, 1), :]
        cos_b, sin_b = cos_ref[nb:nb + rb, :], sin_ref[nb:nb + rb, :]
        lane = lax.broadcasted_iota(jnp.int32, (rb, 128), 1)
        sine = sin_a * cos_b + cos_a * sin_b
        return cos_a * cos_b - sin_a * sin_b, jnp.where(lane < 64, -sine, sine)

    def rotate(x, angles):
        return (x * angles[0] + pltpu.roll(x, 64, 1) * angles[1]).astype(BF16)

    def project_q(b):
        @pl.when(jnp.logical_not(last))
        def _():
            h_load(b).wait()

        @pl.when(b == 0)
        def _():
            wq_load.wait()

        span = block_rows(b, rb)
        normed = normalize(h_buf[span, :].astype(F32), gain_ref[...]).astype(BF16)
        proj = jnp.dot(normed, wq_buf[...], preferred_element_type=F32)
        angles = block_angles(b)
        for head in range(4):
            q_buf[head // 2, (head % 2) * rb:(head % 2 + 1) * rb, :] = rotate(normalize(proj[:, head * 128:(head + 1) * 128], qg_ref[...]), angles)

    def project_new(part):
        rows = 2 * rb
        for b in range(2):
            h_load(2 * part + b).wait()
        span = block_rows(part, rows)
        normed = normalize(h_buf[span, :].astype(F32), gain_ref[...]).astype(BF16)
        proj = jnp.dot(normed, wkv_buf[...], preferred_element_type=F32)
        angles = [jnp.concatenate(pair, axis=0) for pair in zip(block_angles(2 * part), block_angles(2 * part + 1))]
        place = pl.ds(pl.multiple_of(old_len + part * rows, rows), rows)
        heads = []
        for n in range(2):
            heads.append(rotate(normalize(proj[:, n * 128:(n + 1) * 128], kg_ref[...]), angles))
            k_buf[n, place, :] = heads[n]
            v_buf[n, place, :] = proj[:, kv_cols + n * 128:kv_cols + (n + 1) * 128].astype(BF16)
        new_buf[0, span] = jnp.concatenate(heads, axis=1).reshape(rows, 2, 128)
        new_buf[1, span] = proj[:, kv_cols:].astype(BF16).reshape(rows, 2, 128)

    def split_heads(start, stop):
        for src, dst in ((kc_buf, k_buf), (vc_buf, v_buf)):
            for row in range(start, stop, 256):
                x = src[row:row + 256].reshape(256, kv_cols)
                for n in range(2):
                    dst[n, row:row + 256, :] = x[:, n * 128:(n + 1) * 128]

    def prepare_keys(half):
        for load in cache_loads(half):
            load.wait()
        if half == 0:
            split_heads(0, keys // 2)
        else:
            split_heads(keys // 2, old_len)

            @pl.when(jnp.logical_not(last))
            def _():
                split_heads(old_len, keys)

    @pl.when(last)
    def _():
        wk_load.wait()
        wv_load.wait()
        for n in range(2):
            k_buf[n, old_len:keys, :] = jnp.zeros((chunk_len, 128), BF16)
            v_buf[n, old_len:keys, :] = jnp.zeros((chunk_len, 128), BF16)

    def row_copy(kind, b, src, dst, peer):
        return pltpu.make_async_remote_copy(src.at[b], dst.at[b], row_send.at[kind, b], row_recv.at[kind, b], device_id=peer, device_id_type=MESH)

    def sub_copy(kind, b, j, src, dst, peer):
        return pltpu.make_async_remote_copy(src.at[b, j], dst.at[b, j], sub_send.at[kind, b], sub_recv.at[kind, b, j], device_id=peer, device_id_type=MESH)

    copy_a = lambda b: row_copy(0, b, a_send, a_recv, core_peer)
    copy_y = lambda b: row_copy(1, b, y_send, y_recv, y_peer)
    copy_o = lambda b: row_copy(2, b, o_send, o_recv, core_peer)
    copy_p = lambda b, j: sub_copy(0, b, j, p_buf, p_recv, pair_peer)
    copy_m = lambda b, j: sub_copy(1, b, j, m_send, m_recv, cross_peer)
    copy_f = lambda b, j: sub_copy(2, b, j, f_buf, f_buf, pair_peer)
    copy_yf = lambda b, j: sub_copy(3, b, j, f_buf, yf_recv, y_peer)
    copy_d1 = lambda b, j: sub_copy(4, b, j, f_buf, d1_recv, core_peer)
    copy_d2 = lambda b, j: sub_copy(5, b, j, yf_recv, d2_recv, core_peer)

    def sub_sent(kind, b, src, dst, peer):
        pltpu.make_async_remote_copy(src.at[b], dst.at[b], sub_send.at[kind, b], sub_recv.at[kind, b, 0], device_id=peer, device_id_type=MESH).wait_send()

    def columns_of(core, j):
        return pl.ds(pl.multiple_of(core * half_cols + j * sub_cols, sub_cols), sub_cols)

    def attend(b, n, half, width):
        q = q_buf[n]
        row = b * rb + lax.rem(lax.broadcasted_iota(jnp.int32, (2 * rb, 1), 0), rb) + jnp.where(last, 0, keys)
        first = half * (keys // 2)
        scores = lax.dot_general(q, k_buf[n, first:first + width, :], (((1,), (1,)), ((), ())), preferred_element_type=F32)
        parts = []
        for start in range(0, width, chunk_keys):
            s, key = scores[:, start:start + chunk_keys], first + start
            if key >= keys - chunk_len:
                column = key - (keys - chunk_len) + lax.broadcasted_iota(jnp.int32, (1, chunk_keys), 1)
                s = jnp.where(column <= row, s, -jnp.inf)
            elif key > 0:
                s = s + bias_ref[0:1, key:key + chunk_keys]
            parts.append(s)
        m = jnp.max(functools.reduce(jnp.maximum, parts), axis=-1, keepdims=True)
        if half:
            m = jnp.maximum(m, att_m[...])
        weights = [jnp.exp2((s - m) * scale) for s in parts]
        l = jnp.sum(functools.reduce(jnp.add, weights), axis=-1, keepdims=True)
        acc = jnp.dot(jnp.concatenate([p.astype(BF16) for p in weights], axis=1), v_buf[n, first:first + width, :], preferred_element_type=F32)
        if half:
            fade = jnp.exp2((att_m[...] - m) * scale)
            l, acc = att_l[...] * fade + l, att_acc[...] * fade + acc
        if not half:
            att_m[...], att_l[...], att_acc[...] = m, l, acc
        return acc, m, l

    def keep_piece(b, n, head, width):
        acc, m, l = attend(b, n, 1, width)
        tile = stats_tile(rb, [m[:rb], l[:rb], m[rb:], l[rb:]])
        if head:
            own_num[:, 0:128] = acc[:rb]
            own_num[:, 128:256] = acc[rb:]
            own_st[...] = tile
        else:
            a_send[b, :rb, 0:128] = acc[:rb]
            a_send[b, :rb, 128:256] = acc[rb:]
            a_send[b, :, 256:384] = tile
            copy_a(b).start()

    def stage_attend(b, piece):
        head, half = piece // 2, piece % 2
        n = c if head else other_c

        if piece == 0:
            @pl.when(jnp.logical_and(last, lax.rem(b, 2) == 0))
            def _():
                project_new(lax.div(b, 2))

            project_q(b)
        if head == 0:
            @pl.when(b == 0)
            def _():
                prepare_keys(half)

        if not half:
            attend(b, n, half, keys // 2)
            return

        short = jnp.logical_and(last, b < nb // 2)

        @pl.when(short)
        def _():
            keep_piece(b, n, head, keys // 2 - chunk_len // 2)

        @pl.when(jnp.logical_not(short))
        def _():
            keep_piece(b, n, head, keys // 2)

    def stage_core_merge(b):
        copy_a(b).wait_recv()
        nums, columns = merge(own_num[...], own_st[...], a_recv[b, :, 0:256], a_recv[b, :, 256:384], scale)
        tile = stats_tile(rb, columns)
        comb_num[:, 0:128] = nums[0]
        comb_num[:, 128:256] = nums[1]
        comb_st[...] = tile
        mine = pl.ds(pl.multiple_of(y * hb, hb), hb)
        theirs = pl.ds(pl.multiple_of(other_y * hb, hb), hb)
        y_send[b, :hb, :] = comb_num[theirs, :]
        rows8 = stats_rows(tile)
        y_send[b, hb:hb + STAT_ROWS, :] = jnp.concatenate([rows8, rows8], axis=1)
        copy_y(b).start()
        y_num[b] = comb_num[mine, :]
        y_st[b] = comb_st[mine, :]

    def stage_y_merge(b):
        copy_y(b).wait_recv()
        comb_st[...] = stats_columns(y_recv[b, hb:hb + STAT_ROWS, 0:128])
        peer_tile = comb_st[pl.ds(pl.multiple_of(y * hb, hb), hb), :]
        nums, columns = merge(y_num[b], y_st[b], y_recv[b, :hb, :], peer_tile, scale)
        o = jnp.concatenate([nums[0] / columns[1], nums[1] / columns[3]], axis=1).astype(BF16)
        o_send[b] = o.astype(F32)
        copy_o(b).start()
        o_own[b] = o

    def stage_project(b):
        @pl.when(b == 0)
        def _():
            w_load.wait()

        copy_o(b).wait_recv()
        w_mine = w_buf[pl.ds(pl.multiple_of(c * head_cols, head_cols), head_cols), :]
        w_peer = w_buf[pl.ds(pl.multiple_of(other_c * head_cols, head_cols), head_cols), :]
        part = jnp.dot(o_own[b], w_mine, preferred_element_type=F32)
        part = part + jnp.dot(o_recv[b].astype(BF16), w_peer, preferred_element_type=F32)
        for j in range(SUBS):
            p_buf[b, j] = part[:, j * sub_cols:(j + 1) * sub_cols]

        @pl.when(is_end)
        def _():
            for j in range(SUBS):
                copy_p(b, j).start()

    def stage_pair_sum(b, j):
        copy_p(b, j).wait_recv()
        m_send[b, j] = p_buf[b, j] + p_recv[b, j]
        copy_m(b, j).start()

    def stage_total(b, j):
        copy_m(b, j).wait_recv()
        hidden = h_buf[half_rows(b, y), columns_of(c, j)].astype(F32)
        result = (hidden + (m_send[b, j] + m_recv[b, j])).astype(BF16)
        f_buf[b, j] = result.astype(F32)
        copy_f(b, j).start()
        copy_yf(b, j).start()
        copy_d1(b, j).start()
        out_buf[half_rows(b, y), columns_of(c, j)] = result

    def stage_end_total(b, j):
        copy_f(b, j).wait_recv()
        copy_yf(b, j).start()
        copy_d1(b, j).start()
        out_buf[half_rows(b, y), columns_of(c, j)] = f_buf[b, j].astype(BF16)

    def stage_y_total(b, j):
        copy_yf(b, j).wait_recv()
        copy_d2(b, j).start()
        out_buf[half_rows(b, other_y), columns_of(c, j)] = yf_recv[b, j].astype(BF16)

    def stage_store(b, j):
        copy_d1(b, j).wait_recv()
        out_buf[half_rows(b, y), columns_of(other_c, j)] = d1_recv[b, j].astype(BF16)
        copy_d2(b, j).wait_recv()
        out_buf[half_rows(b, other_y), columns_of(other_c, j)] = d2_recv[b, j].astype(BF16)

    def stage_sent(b):
        for sent in (copy_a, copy_y, copy_o):
            sent(b).wait_send()
        sub_sent(3, b, f_buf, yf_recv, y_peer)
        sub_sent(4, b, f_buf, d1_recv, core_peer)
        sub_sent(5, b, yf_recv, d2_recv, core_peer)

        @pl.when(is_mid)
        def _():
            sub_sent(1, b, m_send, m_recv, cross_peer)
            sub_sent(2, b, f_buf, f_buf, pair_peer)

        @pl.when(is_end)
        def _():
            sub_sent(0, b, p_buf, p_recv, pair_peer)

    def run(stage, it, step, lag, guard=None, sub=True):
        j = (step - lag) % SUBS
        if not sub and j:
            return
        b = it + (step - lag - j) // SUBS
        live = jnp.logical_and(b >= 0, b < nb)
        if guard is not None:
            live = jnp.logical_and(live, guard)

        @pl.when(live)
        def _():
            if sub:
                stage(b, j)
            else:
                stage(b)

    lag_p = LAG_PROJECT + LAG_P
    lag_m = lag_p + LAG_M
    lag_f = lag_m + LAG_F
    lag_store = lag_f + LAG_YF + 2

    def body(it, carry):
        for step in range(SUBS):
            run(stage_store, it, step, lag_store)
            run(stage_y_total, it, step, lag_f + LAG_YF, is_end)
            run(stage_end_total, it, step, lag_f, is_end)
            run(stage_y_total, it, step, lag_m + LAG_YF, is_mid)
            run(stage_total, it, step, lag_m, is_mid)
            run(stage_pair_sum, it, step, lag_p, is_mid)
            if step % PIECE_STEPS == 0:
                run(lambda b, j: stage_attend(b, j // PIECE_STEPS), it, step, 0)
            run(stage_core_merge, it, step, 3 * PIECE_STEPS, sub=False)
            run(stage_y_merge, it, step, LAG_Y, sub=False)
            run(stage_project, it, step, LAG_PROJECT, sub=False)
        return carry

    lax.fori_loop(0, nb + (lag_store + SUBS - 1) // SUBS, body, 0)
    lax.fori_loop(0, nb, lambda b, carry: (stage_sent(b), carry)[1], 0)


def finish_kernel(pos_ref, kc_buf, vc_buf, new_buf, x_buf, kc_out, vc_out, x_out, sems):
    is_last = lax.axis_index("sp") == LAST_SHARD
    shard_len, chunk_len = kc_buf.shape[0], new_buf.shape[1]
    write_at = jnp.clip(pos_ref[0] - LAST_SHARD * shard_len, 0, shard_len - chunk_len)
    span = pl.ds(write_at, chunk_len)
    k_store = pltpu.make_async_copy(kc_buf, kc_out, sems.at[0])
    v_store = pltpu.make_async_copy(vc_buf, vc_out, sems.at[1])
    x_store = pltpu.make_async_copy(x_buf, x_out, sems.at[2])
    new_stores = (pltpu.make_async_copy(new_buf.at[0], kc_out.at[span], sems.at[3]), pltpu.make_async_copy(new_buf.at[1], vc_out.at[span], sems.at[4]))
    k_store.start()
    v_store.start()
    x_store.start()
    k_store.wait()
    v_store.wait()

    @pl.when(is_last)
    def _():
        for store in new_stores:
            store.start()
        for store in new_stores:
            store.wait()

    x_store.wait()


def finish_call(start_pos, k_old, v_old, new_rows, result):
    hbm = pl.BlockSpec(memory_space=pl.ANY)
    vmem = pl.BlockSpec(memory_space=pltpu.VMEM)
    shapes = [jax.ShapeDtypeStruct(x.shape, x.dtype) for x in (k_old, v_old, result)]
    return pl.pallas_call(
        finish_kernel,
        out_shape=tuple(shapes),
        in_specs=[pl.BlockSpec(memory_space=pltpu.SMEM)] + [vmem] * 4,
        out_specs=(hbm, hbm, hbm),
        scratch_shapes=[pltpu.SemaphoreType.DMA((5,))],
        compiler_params=pltpu.CompilerParams(vmem_limit_bytes=2 * 2**20),
        name="finish",
    )(start_pos, k_old, v_old, new_rows, result)


def attend_call(start_pos, hidden, norm_gain, w_query, w_key, w_value, q_gain, k_gain, cosine, sine, k_shard, v_shard, w_out, chunk_keys, scale, z_count):
    chunk_len, model_dim = hidden.shape
    keys, kv_local, head_dim = k_shard.shape
    rb = ROW_BLOCK
    nb, hb = chunk_len // rb, rb // 2
    half_cols = model_dim // 2
    heads = w_out.shape[0] // 2
    cfg = (nb, rb, keys, chunk_keys, chunk_len, scale, z_count)
    sub = pltpu.VMEM((nb, SUBS, hb, half_cols // SUBS), F32)
    flops = 4 * 4 * chunk_len * keys * 128 + 2 * chunk_len * w_out.shape[0] * model_dim // 4
    vmem = pl.BlockSpec(memory_space=pltpu.VMEM)
    hbm = pl.BlockSpec(memory_space=pl.ANY)
    outs = (pltpu.VMEM((chunk_len, model_dim), BF16), pltpu.VMEM(k_shard.shape, BF16), pltpu.VMEM(k_shard.shape, BF16),
            pltpu.VMEM((2, chunk_len, kv_local, head_dim), BF16))
    return pl.pallas_call(
        functools.partial(attend_kernel, cfg),
        out_shape=outs,
        in_specs=[pl.BlockSpec(memory_space=pltpu.SMEM), hbm, vmem, hbm, hbm, hbm, vmem, vmem, vmem, vmem, hbm, hbm, hbm],
        out_specs=(vmem, vmem, vmem, vmem),
        scratch_shapes=[
            pltpu.VMEM((chunk_len, model_dim), BF16),
            pltpu.VMEM(w_query.shape, BF16),
            pltpu.VMEM((model_dim, 2 * w_key.shape[1]), BF16),
            pltpu.VMEM((kv_local, keys, head_dim), BF16),
            pltpu.VMEM((kv_local, keys, head_dim), BF16),
            pltpu.VMEM((kv_local, 2 * rb, head_dim), BF16),
            pltpu.VMEM((1, keys), F32),
            pltpu.VMEM((w_out.shape[0], half_cols), BF16),
            pltpu.VMEM((2 * rb, 1), F32),
            pltpu.VMEM((2 * rb, 1), F32),
            pltpu.VMEM((2 * rb, 128), F32),
            pltpu.VMEM((nb, rb, heads + 128), F32),
            pltpu.VMEM((nb, rb, heads + 128), F32),
            pltpu.VMEM((rb, heads), F32),
            pltpu.VMEM((rb, 128), F32),
            pltpu.VMEM((rb, heads), F32),
            pltpu.VMEM((rb, 128), F32),
            pltpu.VMEM((nb, hb + STAT_ROWS, heads), F32),
            pltpu.VMEM((nb, hb + STAT_ROWS, heads), F32),
            pltpu.VMEM((nb, hb, heads), F32),
            pltpu.VMEM((nb, hb, 128), F32),
            pltpu.VMEM((nb, hb, heads), BF16),
            pltpu.VMEM((nb, hb, heads), F32),
            pltpu.VMEM((nb, hb, heads), F32),
            sub, sub, sub, sub, sub, sub, sub, sub,
            pltpu.SemaphoreType.DMA((3, nb)),
            pltpu.SemaphoreType.DMA((3, nb)),
            pltpu.SemaphoreType.DMA((6, nb)),
            pltpu.SemaphoreType.DMA((6, nb, SUBS)),
            pltpu.SemaphoreType.DMA((2, 2)),
            pltpu.SemaphoreType.DMA((4,)),
            pltpu.SemaphoreType.DMA((nb,)),
        ],
        compiler_params=pltpu.CompilerParams(collective_id=0, has_side_effects=True, vmem_limit_bytes=ATTEND_VMEM * 2**20),
        cost_estimate=pl.CostEstimate(flops=flops, bytes_accessed=16 * 2**20, transcendentals=4 * chunk_len * keys),
        name="attend",
    )(start_pos, hidden, norm_gain[None, :], w_query, w_key, w_value, q_gain[None, :], k_gain[None, :], cosine, sine, k_shard, v_shard, w_out)


def solution(mesh, chunk_keys=512):
    cache_spec = P(("dp", "sp"), "tp", None)
    in_specs = (P("dp", None), P("dp"), cache_spec, cache_spec, P(None), P(None, "tp"), P(None, "tp"), P(None, "tp"), P(None), P(None), P("tp", None))
    out_specs = (P("dp", None), cache_spec, cache_spec)

    def local_step(hidden, start_pos, k_shard, v_shard, norm_gain, w_query, w_key, w_value, q_gain, k_gain, w_out):
        chunk_len, model_dim = hidden.shape
        shard_len, kv_local, head_dim = k_shard.shape
        cosine, sine = rotary_tables(start_pos[0], chunk_len, head_dim)
        scale = LOG2E * head_dim ** -0.5
        result, k_old, v_old, new_rows = attend_call(start_pos, hidden, norm_gain, w_query, w_key, w_value, q_gain, k_gain, cosine, sine, k_shard, v_shard, w_out,
                                           chunk_keys, scale, mesh.shape["tp"])
        k_upd, v_upd, out = finish_call(start_pos, k_old, v_old, new_rows, result)
        return out, k_upd, v_upd

    return jax.shard_map(local_step, mesh=mesh, in_specs=in_specs, out_specs=out_specs, check_vma=False)
```

```python
import functools

import jax
import jax.numpy as jnp
from jax import lax
from jax.experimental import pallas as pl
from jax.experimental.pallas import tpu as pltpu
from jax.sharding import PartitionSpec as P

ROPE_BASE = 1e6
NORM_EPS = 1e-6
LOG2E = 1.4426950408889634
MESH = pl.DeviceIdType.MESH
F32 = jnp.float32
BF16 = jnp.bfloat16
ROW_BLOCK = 128
STAT_ROWS = 8
SUBS = 4
PIECE_STEPS = SUBS // 4
LAG_Y = 6
LAG_PROJECT = 7
LAG_P = 3
LAG_M = 3
LAG_F = 3
LAG_YF = 4
LAST_SHARD = 3
ATTEND_VMEM = 50


def rotary_tables(first_pos, chunk_len, head_dim):
    half_dim = head_dim // 2
    inv_freq = ROPE_BASE ** (-2.0 * jnp.arange(half_dim, dtype=jnp.float32) / head_dim)
    starts = first_pos + ROW_BLOCK * jnp.arange(chunk_len // ROW_BLOCK, dtype=jnp.int32)
    places = jnp.concatenate([starts, jnp.arange(ROW_BLOCK, dtype=jnp.int32)])
    angles = places.astype(jnp.float32)[:, None] * jnp.tile(inv_freq, 2)[None, :]
    return jnp.cos(angles), jnp.sin(angles)


def stats_tile(rows, columns):
    lane = lax.broadcasted_iota(jnp.int32, (rows, 128), 1)
    tile = jnp.zeros((rows, 128), F32)
    for k, column in enumerate(columns):
        tile = jnp.where(lane == k, column, tile)
    return tile


def stats_rows(tile):
    return jnp.transpose(tile)[:STAT_ROWS]


def stats_columns(rows8):
    return jnp.transpose(jnp.concatenate([rows8] * (128 // STAT_ROWS), axis=0))


def merge(num_a, tile_a, num_b, tile_b, scale):
    nums, columns = [], []
    for g in range(2):
        m_a, l_a = tile_a[:, 2 * g:2 * g + 1], tile_a[:, 2 * g + 1:2 * g + 2]
        m_b, l_b = tile_b[:, 2 * g:2 * g + 1], tile_b[:, 2 * g + 1:2 * g + 2]
        m = jnp.maximum(m_a, m_b)
        c_a = jnp.exp2((m_a - m) * scale)
        c_b = jnp.exp2((m_b - m) * scale)
        nums.append(num_a[:, g * 128:(g + 1) * 128] * c_a + num_b[:, g * 128:(g + 1) * 128] * c_b)
        columns += [m, l_a * c_a + l_b * c_b]
    return nums, columns


def attend_kernel(cfg, pos_ref, h_hbm, gain_ref, wq_hbm, wk_hbm, wv_hbm, qg_ref, kg_ref, cos_ref, sin_ref, kc_hbm, vc_hbm, w_hbm, out_buf, kc_buf, vc_buf, new_buf,
                  h_buf, wq_buf, wkv_buf, k_buf, v_buf, q_buf, bias_ref, w_buf, att_m, att_l, att_acc,
                  a_send, a_recv, own_num, own_st, comb_num, comb_st, y_send, y_recv, y_num, y_st, o_own, o_send, o_recv,
                  p_buf, p_recv, m_send, m_recv, f_buf, yf_recv, d1_recv, d2_recv, row_send, row_recv, sub_send, sub_recv,
                  kv_sems, w_sems, h_sems):
    nb, rb, keys, chunk_keys, chunk_len, scale, z_count = cfg
    hb = rb // 2
    dp, z, sp = lax.axis_index("dp"), lax.axis_index("tp"), lax.axis_index("sp")
    y, c = lax.div(sp, 2), lax.rem(sp, 2)
    other_y, other_c = 1 - y, 1 - c
    pair_z = z + 1 - 2 * lax.rem(z, 2)
    cross_z = z_count - 1 - z
    is_mid = jnp.logical_and(z >= 1, z <= 2)
    is_end = jnp.logical_not(is_mid)
    half_cols = w_buf.shape[1]
    sub_cols = half_cols // SUBS
    head_cols = w_buf.shape[0] // 2
    core_peer = (dp, z, y * 2 + other_c)
    y_peer = (dp, z, other_y * 2 + c)
    pair_peer = (dp, pair_z, sp)
    cross_peer = (dp, cross_z, sp)
    my_cols = pl.ds(pl.multiple_of(c * half_cols, half_cols), half_cols)

    last = sp == LAST_SHARD
    old_len = keys - chunk_len
    kv_cols = wk_hbm.shape[1]
    limit = jnp.where(last, pos_ref[0] - LAST_SHARD * keys, keys)

    def half_rows(b, which):
        return pl.ds(pl.multiple_of(b * rb + which * hb, hb), hb)

    def block_rows(b, rows):
        return pl.ds(pl.multiple_of(b * rows, rows), rows)

    def cache_loads(half):
        span = pl.ds(half * (keys // 2), keys // 2)
        return (pltpu.make_async_copy(kc_hbm.at[span], kc_buf.at[span], kv_sems.at[0, half]),
                pltpu.make_async_copy(vc_hbm.at[span], vc_buf.at[span], kv_sems.at[1, half]))

    def h_load(b):
        return pltpu.make_async_copy(h_hbm.at[block_rows(b, rb)], h_buf.at[block_rows(b, rb)], h_sems.at[b])

    wq_load = pltpu.make_async_copy(wq_hbm, wq_buf, w_sems.at[0])
    wk_load = pltpu.make_async_copy(wk_hbm, wkv_buf.at[:, pl.ds(0, kv_cols)], w_sems.at[1])
    wv_load = pltpu.make_async_copy(wv_hbm, wkv_buf.at[:, pl.ds(kv_cols, kv_cols)], w_sems.at[2])
    w_load = pltpu.make_async_copy(w_hbm.at[:, my_cols], w_buf, w_sems.at[3])

    @pl.when(last)
    def _():
        wk_load.start()
        wv_load.start()

    h_load(0).start()
    h_load(1).start()
    wq_load.start()
    for half in range(2):
        for load in cache_loads(half):
            load.start()
    for b in range(2, nb):
        h_load(b).start()
    w_load.start()

    barrier = pltpu.get_barrier_semaphore()
    for peer in (core_peer, y_peer, pair_peer):
        pl.semaphore_signal(barrier, inc=1, device_id=peer, device_id_type=MESH)

    @pl.when(is_mid)
    def _():
        pl.semaphore_signal(barrier, inc=1, device_id=cross_peer, device_id_type=MESH)
        pl.semaphore_wait(barrier, 4)

    @pl.when(is_end)
    def _():
        pl.semaphore_wait(barrier, 3)

    key_index = lax.broadcasted_iota(jnp.int32, (1, keys), 1)
    bias_ref[...] = jnp.where(key_index < limit, 0.0, -jnp.inf).astype(F32)

    def normalize(x, gain):
        return x * lax.rsqrt(jnp.mean(x * x, axis=-1, keepdims=True) + NORM_EPS) * gain

    def block_angles(b):
        cos_a, sin_a = cos_ref[pl.ds(b, 1), :], sin_ref[pl.ds(b, 1), :]
        cos_b, sin_b = cos_ref[nb:nb + rb, :], sin_ref[nb:nb + rb, :]
        lane = lax.broadcasted_iota(jnp.int32, (rb, 128), 1)
        sine = sin_a * cos_b + cos_a * sin_b
        return cos_a * cos_b - sin_a * sin_b, jnp.where(lane < 64, -sine, sine)

    def rotate(x, angles):
        return (x * angles[0] + pltpu.roll(x, 64, 1) * angles[1]).astype(BF16)

    def project_q(b):
        @pl.when(jnp.logical_not(last))
        def _():
            h_load(b).wait()

        @pl.when(b == 0)
        def _():
            wq_load.wait()

        span = block_rows(b, rb)
        normed = normalize(h_buf[span, :].astype(F32), gain_ref[...]).astype(BF16)
        proj = jnp.dot(normed, wq_buf[...], preferred_element_type=F32)
        angles = block_angles(b)
        for head in range(4):
            q_buf[head // 2, (head % 2) * rb:(head % 2 + 1) * rb, :] = rotate(normalize(proj[:, head * 128:(head + 1) * 128], qg_ref[...]), angles)

    def project_new(part):
        rows = 2 * rb
        for b in range(2):
            h_load(2 * part + b).wait()
        span = block_rows(part, rows)
        normed = normalize(h_buf[span, :].astype(F32), gain_ref[...]).astype(BF16)
        proj = jnp.dot(normed, wkv_buf[...], preferred_element_type=F32)
        angles = [jnp.concatenate(pair, axis=0) for pair in zip(block_angles(2 * part), block_angles(2 * part + 1))]
        place = pl.ds(pl.multiple_of(old_len + part * rows, rows), rows)
        heads = []
        for n in range(2):
            heads.append(rotate(normalize(proj[:, n * 128:(n + 1) * 128], kg_ref[...]), angles))
            k_buf[n, place, :] = heads[n]
            v_buf[n, place, :] = proj[:, kv_cols + n * 128:kv_cols + (n + 1) * 128].astype(BF16)
        new_buf[0, span] = jnp.concatenate(heads, axis=1).reshape(rows, 2, 128)
        new_buf[1, span] = proj[:, kv_cols:].astype(BF16).reshape(rows, 2, 128)

    def split_heads(start, stop):
        for src, dst in ((kc_buf, k_buf), (vc_buf, v_buf)):
            for row in range(start, stop, 256):
                x = src[row:row + 256].reshape(256, kv_cols)
                for n in range(2):
                    dst[n, row:row + 256, :] = x[:, n * 128:(n + 1) * 128]

    def prepare_keys(half):
        for load in cache_loads(half):
            load.wait()
        if half == 0:
            split_heads(0, keys // 2)
        else:
            split_heads(keys // 2, old_len)

            @pl.when(jnp.logical_not(last))
            def _():
                split_heads(old_len, keys)

    @pl.when(last)
    def _():
        wk_load.wait()
        wv_load.wait()
        for n in range(2):
            k_buf[n, old_len:keys, :] = jnp.zeros((chunk_len, 128), BF16)
            v_buf[n, old_len:keys, :] = jnp.zeros((chunk_len, 128), BF16)

    def row_copy(kind, b, src, dst, peer):
        return pltpu.make_async_remote_copy(src.at[b], dst.at[b], row_send.at[kind, b], row_recv.at[kind, b], device_id=peer, device_id_type=MESH)

    def sub_copy(kind, b, j, src, dst, peer):
        return pltpu.make_async_remote_copy(src.at[b, j], dst.at[b, j], sub_send.at[kind, b], sub_recv.at[kind, b, j], device_id=peer, device_id_type=MESH)

    copy_a = lambda b: row_copy(0, b, a_send, a_recv, core_peer)
    copy_y = lambda b: row_copy(1, b, y_send, y_recv, y_peer)
    copy_o = lambda b: row_copy(2, b, o_send, o_recv, core_peer)
    copy_p = lambda b, j: sub_copy(0, b, j, p_buf, p_recv, pair_peer)
    copy_m = lambda b, j: sub_copy(1, b, j, m_send, m_recv, cross_peer)
    copy_f = lambda b, j: sub_copy(2, b, j, f_buf, f_buf, pair_peer)
    copy_yf = lambda b, j: sub_copy(3, b, j, f_buf, yf_recv, y_peer)
    copy_d1 = lambda b, j: sub_copy(4, b, j, f_buf, d1_recv, core_peer)
    copy_d2 = lambda b, j: sub_copy(5, b, j, yf_recv, d2_recv, core_peer)

    def sub_sent(kind, b, src, dst, peer):
        pltpu.make_async_remote_copy(src.at[b], dst.at[b], sub_send.at[kind, b], sub_recv.at[kind, b, 0], device_id=peer, device_id_type=MESH).wait_send()

    def columns_of(core, j):
        return pl.ds(pl.multiple_of(core * half_cols + j * sub_cols, sub_cols), sub_cols)

    def attend(b, n, half, width):
        q = q_buf[n]
        row = b * rb + lax.rem(lax.broadcasted_iota(jnp.int32, (2 * rb, 1), 0), rb) + jnp.where(last, 0, keys)
        first = half * (keys // 2)
        scores = lax.dot_general(q, k_buf[n, first:first + width, :], (((1,), (1,)), ((), ())), preferred_element_type=F32)
        parts = []
        for start in range(0, width, chunk_keys):
            s, key = scores[:, start:start + chunk_keys], first + start
            if key >= keys - chunk_len:
                column = key - (keys - chunk_len) + lax.broadcasted_iota(jnp.int32, (1, chunk_keys), 1)
                s = jnp.where(column <= row, s, -jnp.inf)
            elif key > 0:
                s = s + bias_ref[0:1, key:key + chunk_keys]
            parts.append(s)
        m = jnp.max(functools.reduce(jnp.maximum, parts), axis=-1, keepdims=True)
        if half:
            m = jnp.maximum(m, att_m[...])
        weights = [jnp.exp2((s - m) * scale) for s in parts]
        l = jnp.sum(functools.reduce(jnp.add, weights), axis=-1, keepdims=True)
        acc = jnp.dot(jnp.concatenate([p.astype(BF16) for p in weights], axis=1), v_buf[n, first:first + width, :], preferred_element_type=F32)
        if half:
            fade = jnp.exp2((att_m[...] - m) * scale)
            l, acc = att_l[...] * fade + l, att_acc[...] * fade + acc
        if not half:
            att_m[...], att_l[...], att_acc[...] = m, l, acc
        return acc, m, l

    def keep_piece(b, n, head, width):
        acc, m, l = attend(b, n, 1, width)
        tile = stats_tile(rb, [m[:rb], l[:rb], m[rb:], l[rb:]])
        if head:
            own_num[:, 0:128] = acc[:rb]
            own_num[:, 128:256] = acc[rb:]
            own_st[...] = tile
        else:
            a_send[b, :rb, 0:128] = acc[:rb]
            a_send[b, :rb, 128:256] = acc[rb:]
            a_send[b, :, 256:384] = tile
            copy_a(b).start()

    def stage_attend(b, piece):
        head, half = piece // 2, piece % 2
        n = c if head else other_c

        if piece == 0:
            @pl.when(jnp.logical_and(last, lax.rem(b, 2) == 0))
            def _():
                project_new(lax.div(b, 2))

            project_q(b)
        if head == 0:
            @pl.when(b == 0)
            def _():
                prepare_keys(half)

        if not half:
            attend(b, n, half, keys // 2)
            return

        short = jnp.logical_and(last, b < nb // 2)

        @pl.when(short)
        def _():
            keep_piece(b, n, head, keys // 2 - chunk_len // 2)

        @pl.when(jnp.logical_not(short))
        def _():
            keep_piece(b, n, head, keys // 2)

    def stage_core_merge(b):
        copy_a(b).wait_recv()
        nums, columns = merge(own_num[...], own_st[...], a_recv[b, :, 0:256], a_recv[b, :, 256:384], scale)
        tile = stats_tile(rb, columns)
        comb_num[:, 0:128] = nums[0]
        comb_num[:, 128:256] = nums[1]
        comb_st[...] = tile
        mine = pl.ds(pl.multiple_of(y * hb, hb), hb)
        theirs = pl.ds(pl.multiple_of(other_y * hb, hb), hb)
        y_send[b, :hb, :] = comb_num[theirs, :]
        rows8 = stats_rows(tile)
        y_send[b, hb:hb + STAT_ROWS, :] = jnp.concatenate([rows8, rows8], axis=1)
        copy_y(b).start()
        y_num[b] = comb_num[mine, :]
        y_st[b] = comb_st[mine, :]

    def stage_y_merge(b):
        copy_y(b).wait_recv()
        comb_st[...] = stats_columns(y_recv[b, hb:hb + STAT_ROWS, 0:128])
        peer_tile = comb_st[pl.ds(pl.multiple_of(y * hb, hb), hb), :]
        nums, columns = merge(y_num[b], y_st[b], y_recv[b, :hb, :], peer_tile, scale)
        o = jnp.concatenate([nums[0] / columns[1], nums[1] / columns[3]], axis=1).astype(BF16)
        o_send[b] = o.astype(F32)
        copy_o(b).start()
        o_own[b] = o

    def stage_project(b):
        @pl.when(b == 0)
        def _():
            w_load.wait()

        copy_o(b).wait_recv()
        w_mine = w_buf[pl.ds(pl.multiple_of(c * head_cols, head_cols), head_cols), :]
        w_peer = w_buf[pl.ds(pl.multiple_of(other_c * head_cols, head_cols), head_cols), :]
        part = jnp.dot(o_own[b], w_mine, preferred_element_type=F32)
        part = part + jnp.dot(o_recv[b].astype(BF16), w_peer, preferred_element_type=F32)
        for j in range(SUBS):
            p_buf[b, j] = part[:, j * sub_cols:(j + 1) * sub_cols]

        @pl.when(is_end)
        def _():
            for j in range(SUBS):
                copy_p(b, j).start()

    def stage_pair_sum(b, j):
        copy_p(b, j).wait_recv()
        m_send[b, j] = p_buf[b, j] + p_recv[b, j]
        copy_m(b, j).start()

    def stage_total(b, j):
        copy_m(b, j).wait_recv()
        hidden = h_buf[half_rows(b, y), columns_of(c, j)].astype(F32)
        result = (hidden + (m_send[b, j] + m_recv[b, j])).astype(BF16)
        f_buf[b, j] = result.astype(F32)
        copy_f(b, j).start()
        copy_yf(b, j).start()
        copy_d1(b, j).start()
        out_buf[half_rows(b, y), columns_of(c, j)] = result

    def stage_end_total(b, j):
        copy_f(b, j).wait_recv()
        copy_yf(b, j).start()
        copy_d1(b, j).start()
        out_buf[half_rows(b, y), columns_of(c, j)] = f_buf[b, j].astype(BF16)

    def stage_y_total(b, j):
        copy_yf(b, j).wait_recv()
        copy_d2(b, j).start()
        out_buf[half_rows(b, other_y), columns_of(c, j)] = yf_recv[b, j].astype(BF16)

    def stage_store(b, j):
        copy_d1(b, j).wait_recv()
        out_buf[half_rows(b, y), columns_of(other_c, j)] = d1_recv[b, j].astype(BF16)
        copy_d2(b, j).wait_recv()
        out_buf[half_rows(b, other_y), columns_of(other_c, j)] = d2_recv[b, j].astype(BF16)

    def stage_sent(b):
        for sent in (copy_a, copy_y, copy_o):
            sent(b).wait_send()
        sub_sent(3, b, f_buf, yf_recv, y_peer)
        sub_sent(4, b, f_buf, d1_recv, core_peer)
        sub_sent(5, b, yf_recv, d2_recv, core_peer)

        @pl.when(is_mid)
        def _():
            sub_sent(1, b, m_send, m_recv, cross_peer)
            sub_sent(2, b, f_buf, f_buf, pair_peer)

        @pl.when(is_end)
        def _():
            sub_sent(0, b, p_buf, p_recv, pair_peer)

    def run(stage, it, step, lag, guard=None, sub=True):
        j = (step - lag) % SUBS
        if not sub and j:
            return
        b = it + (step - lag - j) // SUBS
        live = jnp.logical_and(b >= 0, b < nb)
        if guard is not None:
            live = jnp.logical_and(live, guard)

        @pl.when(live)
        def _():
            if sub:
                stage(b, j)
            else:
                stage(b)

    lag_p = LAG_PROJECT + LAG_P
    lag_m = lag_p + LAG_M
    lag_f = lag_m + LAG_F
    lag_store = lag_f + LAG_YF + 2

    def body(it, carry):
        for step in range(SUBS):
            run(stage_store, it, step, lag_store)
            run(stage_y_total, it, step, lag_f + LAG_YF, is_end)
            run(stage_end_total, it, step, lag_f, is_end)
            run(stage_y_total, it, step, lag_m + LAG_YF, is_mid)
            run(stage_total, it, step, lag_m, is_mid)
            run(stage_pair_sum, it, step, lag_p, is_mid)
            run(stage_y_merge, it, step, LAG_Y, sub=False)
            if step % PIECE_STEPS == 0:
                run(lambda b, j: stage_attend(b, j // PIECE_STEPS), it, step, 0)
            run(stage_core_merge, it, step, 3 * PIECE_STEPS, sub=False)
            run(stage_project, it, step, LAG_PROJECT, sub=False)
        return carry

    lax.fori_loop(0, nb + (lag_store + SUBS - 1) // SUBS, body, 0)
    lax.fori_loop(0, nb, lambda b, carry: (stage_sent(b), carry)[1], 0)


def finish_kernel(pos_ref, kc_buf, vc_buf, new_buf, x_buf, kc_out, vc_out, x_out, sems):
    is_last = lax.axis_index("sp") == LAST_SHARD
    shard_len, chunk_len = kc_buf.shape[0], new_buf.shape[1]
    write_at = jnp.clip(pos_ref[0] - LAST_SHARD * shard_len, 0, shard_len - chunk_len)
    span = pl.ds(write_at, chunk_len)
    k_store = pltpu.make_async_copy(kc_buf, kc_out, sems.at[0])
    v_store = pltpu.make_async_copy(vc_buf, vc_out, sems.at[1])
    x_store = pltpu.make_async_copy(x_buf, x_out, sems.at[2])
    new_stores = (pltpu.make_async_copy(new_buf.at[0], kc_out.at[span], sems.at[3]), pltpu.make_async_copy(new_buf.at[1], vc_out.at[span], sems.at[4]))
    k_store.start()
    v_store.start()
    x_store.start()
    k_store.wait()
    v_store.wait()

    @pl.when(is_last)
    def _():
        for store in new_stores:
            store.start()
        for store in new_stores:
            store.wait()

    x_store.wait()


def finish_call(start_pos, k_old, v_old, new_rows, result):
    hbm = pl.BlockSpec(memory_space=pl.ANY)
    vmem = pl.BlockSpec(memory_space=pltpu.VMEM)
    shapes = [jax.ShapeDtypeStruct(x.shape, x.dtype) for x in (k_old, v_old, result)]
    return pl.pallas_call(
        finish_kernel,
        out_shape=tuple(shapes),
        in_specs=[pl.BlockSpec(memory_space=pltpu.SMEM)] + [vmem] * 4,
        out_specs=(hbm, hbm, hbm),
        scratch_shapes=[pltpu.SemaphoreType.DMA((5,))],
        compiler_params=pltpu.CompilerParams(vmem_limit_bytes=2 * 2**20),
        name="finish",
    )(start_pos, k_old, v_old, new_rows, result)


def attend_call(start_pos, hidden, norm_gain, w_query, w_key, w_value, q_gain, k_gain, cosine, sine, k_shard, v_shard, w_out, chunk_keys, scale, z_count):
    chunk_len, model_dim = hidden.shape
    keys, kv_local, head_dim = k_shard.shape
    rb = ROW_BLOCK
    nb, hb = chunk_len // rb, rb // 2
    half_cols = model_dim // 2
    heads = w_out.shape[0] // 2
    cfg = (nb, rb, keys, chunk_keys, chunk_len, scale, z_count)
    sub = pltpu.VMEM((nb, SUBS, hb, half_cols // SUBS), F32)
    flops = 4 * 4 * chunk_len * keys * 128 + 2 * chunk_len * w_out.shape[0] * model_dim // 4
    vmem = pl.BlockSpec(memory_space=pltpu.VMEM)
    hbm = pl.BlockSpec(memory_space=pl.ANY)
    outs = (pltpu.VMEM((chunk_len, model_dim), BF16), pltpu.VMEM(k_shard.shape, BF16), pltpu.VMEM(k_shard.shape, BF16),
            pltpu.VMEM((2, chunk_len, kv_local, head_dim), BF16))
    return pl.pallas_call(
        functools.partial(attend_kernel, cfg),
        out_shape=outs,
        in_specs=[pl.BlockSpec(memory_space=pltpu.SMEM), hbm, vmem, hbm, hbm, hbm, vmem, vmem, vmem, vmem, hbm, hbm, hbm],
        out_specs=(vmem, vmem, vmem, vmem),
        scratch_shapes=[
            pltpu.VMEM((chunk_len, model_dim), BF16),
            pltpu.VMEM(w_query.shape, BF16),
            pltpu.VMEM((model_dim, 2 * w_key.shape[1]), BF16),
            pltpu.VMEM((kv_local, keys, head_dim), BF16),
            pltpu.VMEM((kv_local, keys, head_dim), BF16),
            pltpu.VMEM((kv_local, 2 * rb, head_dim), BF16),
            pltpu.VMEM((1, keys), F32),
            pltpu.VMEM((w_out.shape[0], half_cols), BF16),
            pltpu.VMEM((2 * rb, 1), F32),
            pltpu.VMEM((2 * rb, 1), F32),
            pltpu.VMEM((2 * rb, 128), F32),
            pltpu.VMEM((nb, rb, heads + 128), F32),
            pltpu.VMEM((nb, rb, heads + 128), F32),
            pltpu.VMEM((rb, heads), F32),
            pltpu.VMEM((rb, 128), F32),
            pltpu.VMEM((rb, heads), F32),
            pltpu.VMEM((rb, 128), F32),
            pltpu.VMEM((nb, hb + STAT_ROWS, heads), F32),
            pltpu.VMEM((nb, hb + STAT_ROWS, heads), F32),
            pltpu.VMEM((nb, hb, heads), F32),
            pltpu.VMEM((nb, hb, 128), F32),
            pltpu.VMEM((nb, hb, heads), BF16),
            pltpu.VMEM((nb, hb, heads), F32),
            pltpu.VMEM((nb, hb, heads), F32),
            sub, sub, sub, sub, sub, sub, sub, sub,
            pltpu.SemaphoreType.DMA((3, nb)),
            pltpu.SemaphoreType.DMA((3, nb)),
            pltpu.SemaphoreType.DMA((6, nb)),
            pltpu.SemaphoreType.DMA((6, nb, SUBS)),
            pltpu.SemaphoreType.DMA((2, 2)),
            pltpu.SemaphoreType.DMA((4,)),
            pltpu.SemaphoreType.DMA((nb,)),
        ],
        compiler_params=pltpu.CompilerParams(collective_id=0, has_side_effects=True, vmem_limit_bytes=ATTEND_VMEM * 2**20),
        cost_estimate=pl.CostEstimate(flops=flops, bytes_accessed=16 * 2**20, transcendentals=4 * chunk_len * keys),
        name="attend",
    )(start_pos, hidden, norm_gain[None, :], w_query, w_key, w_value, q_gain[None, :], k_gain[None, :], cosine, sine, k_shard, v_shard, w_out)


def solution(mesh, chunk_keys=512):
    cache_spec = P(("dp", "sp"), "tp", None)
    in_specs = (P("dp", None), P("dp"), cache_spec, cache_spec, P(None), P(None, "tp"), P(None, "tp"), P(None, "tp"), P(None), P(None), P("tp", None))
    out_specs = (P("dp", None), cache_spec, cache_spec)

    def local_step(hidden, start_pos, k_shard, v_shard, norm_gain, w_query, w_key, w_value, q_gain, k_gain, w_out):
        chunk_len, model_dim = hidden.shape
        shard_len, kv_local, head_dim = k_shard.shape
        cosine, sine = rotary_tables(start_pos[0], chunk_len, head_dim)
        scale = LOG2E * head_dim ** -0.5
        result, k_old, v_old, new_rows = attend_call(start_pos, hidden, norm_gain, w_query, w_key, w_value, q_gain, k_gain, cosine, sine, k_shard, v_shard, w_out,
                                           chunk_keys, scale, mesh.shape["tp"])
        k_upd, v_upd, out = finish_call(start_pos, k_old, v_old, new_rows, result)
        return out, k_upd, v_upd

    return jax.shard_map(local_step, mesh=mesh, in_specs=in_specs, out_specs=out_specs, check_vma=False)
```
